16 devices in a mesh: dp: 2 (over z), fsdp: 8 (over y, x, core).
Axes of the slice: x: 2, y: 2, z: 2, core: 2. Of those that a mesh axis runs over, the one named last changes fastest.
Arguments:
- tok_ids: int32 [48, 512], P(('dp', 'fsdp')), parts along dimension 0
- grad_out: bfloat16 [48, 512, 2048], P(('dp', 'fsdp')), parts along dimension 0
- emb_table: bfloat16 [102400, 2048], P('fsdp')
- norm_gain: bfloat16 [2048], P('fsdp')
- w_query: bfloat16 [2048, 3072], P('fsdp')
- w_kv_down: bfloat16 [2048, 576], P('fsdp')
- kv_gain: bfloat16 [512], P('fsdp')
- w_kv_up: bfloat16 [512, 4096], P('fsdp')
- w_out: bfloat16 [2048, 2048], P('fsdp')
Outputs:
- output 1: bfloat16 [48, 512, 2048], P(('dp', 'fsdp')), parts along dimension 0
- output 2: bfloat16 [204800, 2048], P(('dp', 'fsdp')), parts along dimension 0
- output 3: float32 [4096], P(('dp', 'fsdp')), parts along dimension 0
- output 4: float32 [4096, 3072], P(('dp', 'fsdp')), parts along dimension 0
- output 5: float32 [4096, 576], P(('dp', 'fsdp')), parts along dimension 0
- output 6: float32 [1024], P(('dp', 'fsdp')), parts along dimension 0
- output 7: float32 [1024, 4096], P(('dp', 'fsdp')), parts along dimension 0
- output 8: float32 [4096, 2048], P(('dp', 'fsdp')), parts along dimension 0
There are 2 independent parts. The reference program is written for one: setup_inputs(seed, part) draws one part's arguments, and reference() takes and returns one part's arrays. A program takes and returns all parts, laid end to end along the dimension named above; an argument that names none is the same for every part.
All inputs are finite; a program needn't handle non-finite values.
Results may differ from the reference program's by a relative error of at most 0.0124488.
Values are sent between devices in bfloat16 or wider.
A program may use at most 1 GiB of HBM per device.

```python
import math
import jax
import jax.numpy as jnp
from jax import lax

D_MODEL = 2048
N_HEADS = 16
VOCAB_SIZE = 102400
KV_RANK = 512
BATCH_SEQS = 24
SEQ_LEN = 512
NOPE_DIM = 128
ROPE_DIM = 64
VALUE_DIM = 128
HOT_IDS = 64
ROPE_THETA = 50000.0
RMS_EPS = 1e-6
ATTN_SCALE = (NOPE_DIM + ROPE_DIM) ** -0.5 * (0.1 * math.log(32.0) + 1.0) ** 2


def draw_ids(id_key):
    tok_count = BATCH_SEQS * SEQ_LEN
    kind_key, hot_key, mid_key, any_key = jax.random.split(id_key, 4)
    id_kind = jax.random.randint(kind_key, (tok_count,), 0, 4)
    hot_draw = jax.random.randint(hot_key, (tok_count,), 0, HOT_IDS)
    mid_draw = jax.random.randint(mid_key, (tok_count,), 0, VOCAB_SIZE // 8)
    any_draw = jax.random.randint(any_key, (tok_count,), 0, VOCAB_SIZE)
    tok_list = jnp.where(id_kind == 0, hot_draw, jnp.where(id_kind == 1, mid_draw, any_draw))
    tok_list = tok_list.at[0].set(VOCAB_SIZE - 1).at[1].set(0)
    return tok_list.reshape(BATCH_SEQS, SEQ_LEN).astype(jnp.int32)


def setup_inputs(seed: int = 0, part: int = 0) -> dict:
    base_key = jax.random.key(seed)
    shared = jax.random.split(base_key, 7)
    part_keys = jax.random.split(jax.random.fold_in(base_key, part), 2)
    q_width = N_HEADS * (NOPE_DIM + ROPE_DIM)
    up_width = N_HEADS * (NOPE_DIM + VALUE_DIM)
    o_width = N_HEADS * VALUE_DIM
    emb_table = jax.random.normal(shared[0], (VOCAB_SIZE, D_MODEL), jnp.float32).astype(jnp.bfloat16)
    norm_gain = (1.0 + 0.3 * jax.random.normal(shared[1], (D_MODEL,), jnp.float32)).astype(jnp.bfloat16)
    w_query = (jax.random.normal(shared[2], (D_MODEL, q_width), jnp.float32) * D_MODEL ** -0.5).astype(jnp.bfloat16)
    w_kv_down = (jax.random.normal(shared[3], (D_MODEL, KV_RANK + ROPE_DIM), jnp.float32) * D_MODEL ** -0.5).astype(jnp.bfloat16)
    kv_gain = (1.0 + 0.3 * jax.random.normal(shared[4], (KV_RANK,), jnp.float32)).astype(jnp.bfloat16)
    w_kv_up = (jax.random.normal(shared[5], (KV_RANK, up_width), jnp.float32) * KV_RANK ** -0.5).astype(jnp.bfloat16)
    w_out = (jax.random.normal(shared[6], (o_width, D_MODEL), jnp.float32) * o_width ** -0.5).astype(jnp.bfloat16)
    tok_ids = draw_ids(part_keys[0])
    grad_out = jax.random.normal(part_keys[1], (BATCH_SEQS, SEQ_LEN, D_MODEL), jnp.float32).astype(jnp.bfloat16)
    return {'tok_ids': tok_ids, 'grad_out': grad_out, 'emb_table': emb_table, 'norm_gain': norm_gain, 'w_query': w_query, 'w_kv_down': w_kv_down, 'kv_gain': kv_gain, 'w_kv_up': w_kv_up, 'w_out': w_out}


def rms_scale(in_vals, gain_vec):
    vals_f32 = in_vals.astype(jnp.float32)
    inv_rms = lax.rsqrt(jnp.mean(vals_f32 * vals_f32, axis=-1, keepdims=True) + RMS_EPS)
    return (vals_f32 * inv_rms * gain_vec.astype(jnp.float32)).astype(jnp.bfloat16)


def rope_tables():
    positions = jnp.arange(SEQ_LEN, dtype=jnp.float32)
    inv_freq = ROPE_THETA ** (-2.0 * jnp.arange(ROPE_DIM // 2, dtype=jnp.float32) / ROPE_DIM)
    rot_angle = positions[:, None] * inv_freq[None, :]
    rot_angle = jnp.concatenate([rot_angle, rot_angle], axis=-1)
    return jnp.cos(rot_angle), jnp.sin(rot_angle)


def apply_rope(in_vals, cos_tab, sin_tab):
    half_dim = ROPE_DIM // 2
    vals_f32 = in_vals.astype(jnp.float32)
    turned = jnp.concatenate([-vals_f32[..., half_dim:], vals_f32[..., :half_dim]], axis=-1)
    return (vals_f32 * cos_tab + turned * sin_tab).astype(jnp.bfloat16)


def attend_one(q_seq, pe_seq, kv_seq):
    cos_tab, sin_tab = rope_tables()
    q_rot = apply_rope(q_seq[:, :, NOPE_DIM:], cos_tab[:, None, :], sin_tab[:, None, :])
    k_rot = apply_rope(pe_seq, cos_tab, sin_tab)
    scores = jnp.einsum('shd,thd->hst', q_seq[:, :, :NOPE_DIM].astype(jnp.float32), kv_seq[:, :, :NOPE_DIM].astype(jnp.float32))
    scores = scores + jnp.einsum('shd,td->hst', q_rot.astype(jnp.float32), k_rot.astype(jnp.float32))
    positions = jnp.arange(SEQ_LEN)
    causal = positions[:, None] >= positions[None, :]
    scores = jnp.where(causal[None, :, :], scores * ATTN_SCALE, -1e30)
    attn_probs = jax.nn.softmax(scores, axis=-1).astype(jnp.bfloat16)
    attn_mix = jnp.einsum('hst,thd->shd', attn_probs.astype(jnp.float32), kv_seq[:, :, NOPE_DIM:].astype(jnp.float32))
    return attn_mix.astype(jnp.bfloat16).reshape(SEQ_LEN, N_HEADS * VALUE_DIM)


def block_forward(rows_f32, gain_vec, w_query_f, w_down_f, kv_gain_vec, w_up_f, w_out_f):
    normed = rms_scale(rows_f32, gain_vec)
    q_proj = jnp.dot(normed.astype(jnp.float32), w_query_f, preferred_element_type=jnp.float32).astype(jnp.bfloat16)
    kv_down = jnp.dot(normed.astype(jnp.float32), w_down_f, preferred_element_type=jnp.float32).astype(jnp.bfloat16)
    latent = rms_scale(kv_down[:, :KV_RANK], kv_gain_vec)
    kv_up = jnp.dot(latent.astype(jnp.float32), w_up_f, preferred_element_type=jnp.float32).astype(jnp.bfloat16)
    seq_parts = (q_proj.reshape(BATCH_SEQS, SEQ_LEN, N_HEADS, NOPE_DIM + ROPE_DIM), kv_down[:, KV_RANK:].reshape(BATCH_SEQS, SEQ_LEN, ROPE_DIM), kv_up.reshape(BATCH_SEQS, SEQ_LEN, N_HEADS, NOPE_DIM + VALUE_DIM))
    attn_mix = lax.map(jax.checkpoint(lambda seq_item: attend_one(*seq_item)), seq_parts)
    attn_out = jnp.dot(attn_mix.reshape(BATCH_SEQS * SEQ_LEN, N_HEADS * VALUE_DIM).astype(jnp.float32), w_out_f, preferred_element_type=jnp.float32)
    return rows_f32 + attn_out


def reference(tok_ids, grad_out, emb_table, norm_gain, w_query, w_kv_down, kv_gain, w_kv_up, w_out):
    flat_ids = tok_ids.reshape(BATCH_SEQS * SEQ_LEN)
    rows_f32 = jnp.take(emb_table, flat_ids, axis=0).astype(jnp.float32)
    weight_list = tuple(weight_arr.astype(jnp.float32) for weight_arr in (norm_gain, w_query, w_kv_down, kv_gain, w_kv_up, w_out))
    out_f32, pullback = jax.vjp(block_forward, rows_f32, *weight_list)
    grad_list = pullback(grad_out.reshape(BATCH_SEQS * SEQ_LEN, D_MODEL).astype(jnp.float32))
    grad_table = jax.ops.segment_sum(grad_list[0], flat_ids, num_segments=VOCAB_SIZE).astype(jnp.bfloat16)
    block_out = out_f32.astype(jnp.bfloat16).reshape(BATCH_SEQS, SEQ_LEN, D_MODEL)
    return (block_out, grad_table, grad_list[1], grad_list[2], grad_list[3], grad_list[4], grad_list[5], grad_list[6])
```

```python
import math
import jax
import jax.numpy as jnp
from jax import lax
from jax.experimental import pallas as pl
from jax.experimental.pallas import tpu as pltpu
from jax.sharding import PartitionSpec as P

NOPE_DIM = 128
ROPE_DIM = 64
VALUE_DIM = 128
ROPE_THETA = 50000.0
RMS_EPS = 1e-6
ATTN_SCALE = (NOPE_DIM + ROPE_DIM) ** -0.5 * (0.1 * math.log(32.0) + 1.0) ** 2
ROW_DIMS = (((0,), (0,)), ((), ()))
COL_DIMS = (((1,), (1,)), ((), ()))


def rms_scale(in_vals, gain_vec):
    vals_f32 = in_vals.astype(jnp.float32)
    inv_rms = lax.rsqrt(jnp.mean(vals_f32 * vals_f32, axis=-1, keepdims=True) + RMS_EPS)
    return (vals_f32 * inv_rms * gain_vec).astype(jnp.bfloat16)


def rope_tables(seq_len):
    positions = jnp.arange(seq_len, dtype=jnp.float32)
    inv_freq = ROPE_THETA ** (-2.0 * jnp.arange(ROPE_DIM // 2, dtype=jnp.float32) / ROPE_DIM)
    rot_angle = positions[:, None] * inv_freq[None, :]
    rot_angle = jnp.concatenate([rot_angle, rot_angle], axis=-1)
    return jnp.cos(rot_angle), jnp.sin(rot_angle)


def apply_rope(in_vals, cos_tab, sin_tab):
    half_dim = ROPE_DIM // 2
    vals_f32 = in_vals.astype(jnp.float32)
    turned = jnp.concatenate([-vals_f32[..., half_dim:], vals_f32[..., :half_dim]], axis=-1)
    return (vals_f32 * cos_tab + turned * sin_tab).astype(jnp.bfloat16)


def attend_local(q_proj, pe_raw, kv_up):
    seq_len = q_proj.shape[1]
    cos_tab, sin_tab = rope_tables(seq_len)
    q_rot = apply_rope(q_proj[..., NOPE_DIM:], cos_tab[:, None, :], sin_tab[:, None, :])
    k_rot = apply_rope(pe_raw, cos_tab, sin_tab)
    scores = jnp.einsum('bshd,bthd->bhst', q_proj[..., :NOPE_DIM], kv_up[..., :NOPE_DIM], preferred_element_type=jnp.float32)
    scores = scores + jnp.einsum('bshd,btd->bhst', q_rot, k_rot, preferred_element_type=jnp.float32)
    positions = jnp.arange(seq_len)
    causal = positions[:, None] >= positions[None, :]
    scores = jnp.where(causal, scores * ATTN_SCALE, -1e30)
    attn_probs = jax.nn.softmax(scores, axis=-1).astype(jnp.bfloat16)
    attn_mix = jnp.einsum('bhst,bthd->bshd', attn_probs, kv_up[..., NOPE_DIM:], preferred_element_type=jnp.float32)
    return attn_mix.astype(jnp.bfloat16)


def block_step(tok_rows, grad_rows, full_weights, seq_count):
    gain_vec, w_query, w_kv_down, kv_gain, w_kv_up, w_out = full_weights
    kv_rank = kv_gain.shape[0]
    tok_count = tok_rows.shape[0]
    seq_len = tok_count // seq_count
    rows_f32 = tok_rows.astype(jnp.float32)
    normed = rms_scale(rows_f32, gain_vec.astype(jnp.float32))
    q_proj = jnp.dot(normed, w_query, preferred_element_type=jnp.float32).astype(jnp.bfloat16)
    kv_down = jnp.dot(normed, w_kv_down, preferred_element_type=jnp.float32).astype(jnp.bfloat16)
    latent, latent_pull = jax.vjp(rms_scale, kv_down[:, :kv_rank], kv_gain.astype(jnp.float32))
    kv_up = jnp.dot(latent, w_kv_up, preferred_element_type=jnp.float32).astype(jnp.bfloat16)
    attn_mix, attn_pull = jax.vjp(attend_local, q_proj.reshape(seq_count, seq_len, -1, NOPE_DIM + ROPE_DIM), kv_down[:, kv_rank:].reshape(seq_count, seq_len, ROPE_DIM), kv_up.reshape(seq_count, seq_len, -1, NOPE_DIM + VALUE_DIM))
    mix_rows = attn_mix.reshape(tok_count, -1)
    out_f32 = rows_f32 + jnp.dot(mix_rows, w_out, preferred_element_type=jnp.float32)
    d_w_out = lax.dot_general(mix_rows, grad_rows, ROW_DIMS, preferred_element_type=jnp.float32)
    d_mix = lax.dot_general(grad_rows, w_out, COL_DIMS, preferred_element_type=jnp.float32).astype(jnp.bfloat16)
    d_query, d_pe, d_up = attn_pull(d_mix.reshape(attn_mix.shape))
    d_query = d_query.reshape(tok_count, -1)
    d_up = d_up.reshape(tok_count, -1)
    d_w_kv_up = lax.dot_general(latent, d_up, ROW_DIMS, preferred_element_type=jnp.float32)
    d_latent = lax.dot_general(d_up, w_kv_up, COL_DIMS, preferred_element_type=jnp.float32).astype(jnp.bfloat16)
    d_ckv, d_kv_gain = latent_pull(d_latent)
    d_down = jnp.concatenate([d_ckv, d_pe.reshape(tok_count, ROPE_DIM)], axis=1)
    d_w_kv_down = lax.dot_general(normed, d_down, ROW_DIMS, preferred_element_type=jnp.float32)
    d_w_query = lax.dot_general(normed, d_query, ROW_DIMS, preferred_element_type=jnp.float32)
    d_normed = lax.dot_general(d_query, w_query, COL_DIMS, preferred_element_type=jnp.float32)
    d_normed = d_normed + lax.dot_general(d_down, w_kv_down, COL_DIMS, preferred_element_type=jnp.float32)
    return out_f32.astype(jnp.bfloat16), d_normed.astype(jnp.bfloat16), (d_w_query, d_w_kv_down, d_kv_gain, d_w_kv_up, d_w_out)


BASE_CAP = 160
HEAVY_CAP = 480
GROUP_ROWS = 32
FETCH_SLOTS = 4
OUT_ROWS = 128
STEP_ROWS = 128
RELAY_PARTS = 3
MESH_ID = pl.DeviceIdType.MESH


def shifted_sum(counts):
    size = counts.shape[-1]
    lower = jnp.arange(size)[:, None] < jnp.arange(size)[None, :]
    return jnp.sum(jnp.where(lower, counts[..., :, None], 0), axis=-2)


def owner_cap(owner):
    return BASE_CAP + jnp.where(owner == 0, HEAVY_CAP, 0)


def plan_ids(flat_ids, vocab_dev, n_dev):
    tok_count = flat_ids.shape[0]
    order = jnp.arange(tok_count)
    same_before = (flat_ids[:, None] == flat_ids[None, :]) & (order[:, None] < order[None, :])
    is_first = jnp.logical_not(jnp.any(same_before, axis=0))
    lower = (flat_ids[:, None] < flat_ids[None, :]) & is_first[:, None]
    unique_rank = jnp.sum(lower.astype(jnp.int32), axis=0)
    owner = flat_ids // vocab_dev
    owned = owner[:, None] == jnp.arange(n_dev)[None, :]
    counts = jnp.sum((owned & is_first[:, None]).astype(jnp.int32), axis=0)
    owner_rank = unique_rank - jnp.sum(jnp.where(owned, shifted_sum(counts)[None, :], 0), axis=1)
    hits = (unique_rank[:, None] == order[None, :]) & is_first[:, None]
    unique_ids = jnp.sum(jnp.where(hits, flat_ids[:, None] + 1, 0), axis=0) - 1
    return owner, owner_rank, unique_ids, counts


def slots_of(owner, owner_rank, my_dev, n_dev, turn):
    cap = owner_cap(owner)
    within = owner_rank - turn * cap
    slot = jnp.where(within < BASE_CAP, BASE_CAP * (owner ^ my_dev) + within, BASE_CAP * (n_dev - 1) + within)
    return jnp.where((within >= 0) & (within < cap), slot, -1)


def pick_rows(table, unique_ids, starts, row_base, n_dev):
    vocab_dev, width = table.shape
    list_len = unique_ids.shape[-1]
    dest_rows = BASE_CAP + HEAVY_CAP
    base_groups, heavy_groups = BASE_CAP // GROUP_ROWS, HEAVY_CAP // GROUP_ROWS

    def kernel(ids_s, starts_s, base_s, table_ref, out_ref, fetched, picked, fetch_sem, out_sem):
        base = base_s[0]
        n_groups = n_dev * base_groups + jnp.where(base == 0, n_dev * heavy_groups, 0)

        def place(group):
            late = group - n_dev * base_groups
            is_late = late >= 0
            dest = jnp.where(is_late, late // heavy_groups, group // base_groups)
            row = GROUP_ROWS * jnp.where(is_late, lax.rem(late, heavy_groups) + base_groups, lax.rem(group, base_groups))
            return dest, row

        def id_at(dest, where):
            return ids_s[dest * list_len + jnp.minimum(where, list_len - 1)]

        def start_fetch(group):
            slot = lax.rem(group, FETCH_SLOTS)
            dest, row = place(group)
            first = starts_s[dest] + row
            for i in range(GROUP_ROWS):
                at = jnp.clip(id_at(dest, first + i) - base, 0, vocab_dev - 1)
                tile = pl.multiple_of((at // 8) * 8, 8)
                pltpu.make_async_copy(table_ref.at[pl.ds(tile, 8)], fetched.at[slot, pl.ds(8 * i, 8)], fetch_sem.at[slot]).start()

        def out_copy(group):
            slot = lax.rem(group, 2)
            dest, row = place(group)
            return pltpu.make_async_copy(picked.at[slot], out_ref.at[pl.ds(pl.multiple_of(dest * dest_rows + row, GROUP_ROWS), GROUP_ROWS)], out_sem.at[slot])

        for ahead in range(FETCH_SLOTS - 1):
            start_fetch(jnp.int32(ahead))

        def body(group, carry):
            @pl.when(group + FETCH_SLOTS - 1 < n_groups)
            def _():
                start_fetch(group + FETCH_SLOTS - 1)
            slot = lax.rem(group, FETCH_SLOTS)
            dest, row = place(group)
            first = starts_s[dest] + row
            sublane = lax.broadcasted_iota(jnp.int32, (8, 128), 0)
            wanted = []
            for block in range(GROUP_ROWS // 8):
                part = jnp.zeros((8, 128), jnp.int32)
                for i in range(8):
                    at = jnp.clip(id_at(dest, first + 8 * block + i) - base, 0, vocab_dev - 1)
                    part = jnp.where(sublane == i, 8 * (8 * block + i) + lax.rem(at, 8), part)
                wanted.append(part)
            wanted = jnp.concatenate(wanted, axis=0)
            lane = lax.broadcasted_iota(jnp.int32, (GROUP_ROWS, 128), 1)
            chooser = jnp.concatenate([(wanted == lane).astype(jnp.float32), (wanted == lane + 128).astype(jnp.float32)], axis=1).astype(jnp.bfloat16)
            pltpu.make_async_copy(fetched.at[slot], fetched.at[slot], fetch_sem.at[slot]).wait()

            @pl.when(group >= 2)
            def _():
                out_copy(group - 2).wait()
            picked[lax.rem(group, 2)] = jnp.dot(chooser, fetched[slot], preferred_element_type=jnp.float32).astype(jnp.bfloat16)
            out_copy(group).start()
            return carry

        lax.fori_loop(0, n_groups, body, 0)
        for back in (2, 1):
            out_copy(n_groups - back).wait()

    return pl.pallas_call(
        kernel,
        out_shape=jax.ShapeDtypeStruct((n_dev * dest_rows, width), table.dtype),
        grid_spec=pltpu.PrefetchScalarGridSpec(
            num_scalar_prefetch=3,
            grid=(1,),
            in_specs=[pl.BlockSpec(memory_space=pl.ANY)],
            out_specs=pl.BlockSpec(memory_space=pl.ANY),
            scratch_shapes=[
                pltpu.VMEM((FETCH_SLOTS, 8 * GROUP_ROWS, width), table.dtype),
                pltpu.VMEM((2, GROUP_ROWS, width), table.dtype),
                pltpu.SemaphoreType.DMA((FETCH_SLOTS,)),
                pltpu.SemaphoreType.DMA((2,)),
            ],
        ),
        cost_estimate=pl.CostEstimate(flops=4 * 10**9, bytes_accessed=10**8, transcendentals=0),
        name='pick_rows',
    )(unique_ids.reshape(-1), starts, row_base.reshape(1), table)


def greet_all(my_dev, n_dev):
    barrier = pltpu.get_barrier_semaphore()
    for hop in range(1, n_dev):
        pl.semaphore_signal(barrier, inc=1, device_id={'fsdp': my_dev ^ hop}, device_id_type=MESH_ID)
    pl.semaphore_wait(barrier, n_dev - 1)


def swap_rows(picked, n_dev):
    width = picked.shape[-1]
    dest_rows = BASE_CAP + HEAVY_CAP
    n_slots = n_dev * BASE_CAP + HEAVY_CAP
    heavy_at = n_dev * BASE_CAP
    half = HEAVY_CAP // 2
    part_rows = half // RELAY_PARTS

    def kernel(in_ref, out_ref, relay_ref, local, send_sem, recv_sem, relay_send, relay_recv, local_sem):
        my_dev = lax.axis_index('fsdp')
        greet_all(my_dev, n_dev)

        def send(source, target, dest, sem):
            return pltpu.make_async_remote_copy(src_ref=source, dst_ref=target, send_sem=send_sem.at[sem], recv_sem=recv_sem.at[sem], device_id={'fsdp': dest}, device_id_type=MESH_ID)

        def base_copy(hop):
            dest = my_dev ^ hop
            return send(in_ref.at[pl.ds(pl.multiple_of(dest * dest_rows, 32), BASE_CAP)], out_ref.at[pl.ds(hop * BASE_CAP, BASE_CAP)], dest, hop)

        def heavy_copy(dest):
            rows = half if dest >= 6 else HEAVY_CAP
            return send(in_ref.at[pl.ds(dest * dest_rows + BASE_CAP, rows)], out_ref.at[pl.ds(heavy_at, rows)], jnp.int32(dest), 8)

        def relay_in(dest, part):
            return pltpu.make_async_remote_copy(src_ref=in_ref.at[pl.ds(dest * dest_rows + BASE_CAP + half + part * part_rows, part_rows)], dst_ref=relay_ref.at[pl.ds(part * part_rows, part_rows)], send_sem=relay_send.at[dest - 6, part], recv_sem=relay_recv.at[part], device_id={'fsdp': jnp.int32(dest - 2)}, device_id_type=MESH_ID)

        def relay_out(dest, part):
            return pltpu.make_async_remote_copy(src_ref=relay_ref.at[pl.ds(part * part_rows, part_rows)], dst_ref=out_ref.at[pl.ds(heavy_at + half + part * part_rows, part_rows)], send_sem=relay_send.at[0, part], recv_sem=relay_recv.at[part], device_id={'fsdp': jnp.int32(dest)}, device_id_type=MESH_ID)

        @pl.when(my_dev == 0)
        def _():
            for part in range(RELAY_PARTS):
                for dest in (6, 7):
                    relay_in(dest, part).start()
            for dest in (6, 7, 2, 4, 3, 5, 1):
                rows = half if dest >= 6 else HEAVY_CAP
                pltpu.make_async_remote_copy(src_ref=in_ref.at[pl.ds(dest * dest_rows + BASE_CAP, rows)], dst_ref=out_ref.at[pl.ds(heavy_at, rows)], send_sem=send_sem.at[7 + dest], recv_sem=recv_sem.at[8], device_id={'fsdp': jnp.int32(dest)}, device_id_type=MESH_ID).start()
        for hop in range(1, n_dev):
            base_copy(hop).start()
        own = pltpu.make_async_copy(in_ref.at[pl.ds(pl.multiple_of(my_dev * dest_rows, 32), dest_rows)], local, local_sem.at[0])
        own.start()
        own.wait()
        back = pltpu.make_async_copy(local.at[pl.ds(0, BASE_CAP)], out_ref.at[pl.ds(0, BASE_CAP)], local_sem.at[1])
        back.start()

        @pl.when(my_dev == 0)
        def _():
            mine = pltpu.make_async_copy(local.at[pl.ds(BASE_CAP, HEAVY_CAP)], out_ref.at[pl.ds(heavy_at, HEAVY_CAP)], local_sem.at[2])
            mine.start()
            mine.wait()
        back.wait()
        for mid in (4, 5):
            @pl.when(my_dev == mid)
            def _(mid=mid):
                for part in range(RELAY_PARTS):
                    relay_in(mid + 2, part).wait_recv()
                    relay_out(mid + 2, part).start()
                for part in range(RELAY_PARTS):
                    relay_out(mid + 2, part).wait_send()
        for hop in range(1, n_dev):
            base_copy(hop).wait()
        for dest in range(1, n_dev):
            rows = half if dest >= 6 else HEAVY_CAP

            @pl.when(my_dev == dest)
            def _(dest=dest, rows=rows):
                pltpu.make_async_copy(out_ref.at[pl.ds(heavy_at, rows)], out_ref.at[pl.ds(heavy_at, rows)], recv_sem.at[8]).wait()
                if dest >= 6:
                    for part in range(RELAY_PARTS):
                        relay_out(dest, part).wait_recv()

            @pl.when(my_dev == 0)
            def _(dest=dest, rows=rows):
                pltpu.make_async_copy(in_ref.at[pl.ds(dest * dest_rows + BASE_CAP, rows)], in_ref.at[pl.ds(dest * dest_rows + BASE_CAP, rows)], send_sem.at[7 + dest]).wait()
                if dest >= 6:
                    for part in range(RELAY_PARTS):
                        relay_in(dest, part).wait_send()

    return pl.pallas_call(
        kernel,
        out_shape=(jax.ShapeDtypeStruct((n_slots, width), picked.dtype), jax.ShapeDtypeStruct((half, width), picked.dtype)),
        in_specs=[pl.BlockSpec(memory_space=pl.ANY)],
        out_specs=(pl.BlockSpec(memory_space=pl.ANY),) * 2,
        scratch_shapes=[
            pltpu.VMEM((dest_rows, width), picked.dtype),
            pltpu.SemaphoreType.DMA((15,)),
            pltpu.SemaphoreType.DMA((9,)),
            pltpu.SemaphoreType.DMA((2, RELAY_PARTS)),
            pltpu.SemaphoreType.DMA((RELAY_PARTS,)),
            pltpu.SemaphoreType.DMA((3,)),
        ],
        compiler_params=pltpu.CompilerParams(collective_id=1, has_side_effects=True),
        cost_estimate=pl.CostEstimate(flops=10**9, bytes_accessed=10**8, transcendentals=0),
        name='swap_rows',
    )(picked)[0]


def return_rows(slot_grads, n_dev):
    n_slots, width = slot_grads.shape
    heavy_at = n_dev * BASE_CAP
    half = HEAVY_CAP // 2
    part_rows = half // RELAY_PARTS
    n_rows = n_dev * (BASE_CAP + HEAVY_CAP)

    def kernel(in_ref, out_ref, relay_ref, local, send_sem, recv_sem, relay_send, relay_recv, local_sem):
        my_dev = lax.axis_index('fsdp')
        greet_all(my_dev, n_dev)

        def base_copy(hop):
            return pltpu.make_async_remote_copy(src_ref=in_ref.at[pl.ds(hop * BASE_CAP, BASE_CAP)], dst_ref=out_ref.at[pl.ds(hop * BASE_CAP, BASE_CAP)], send_sem=send_sem.at[hop], recv_sem=recv_sem.at[hop], device_id={'fsdp': my_dev ^ hop}, device_id_type=MESH_ID)

        def heavy_copy(source):
            rows = half if source >= 6 else HEAVY_CAP
            return pltpu.make_async_remote_copy(src_ref=in_ref.at[pl.ds(heavy_at, rows)], dst_ref=out_ref.at[pl.ds(heavy_at + source * HEAVY_CAP, rows)], send_sem=send_sem.at[8], recv_sem=recv_sem.at[7 + source], device_id={'fsdp': jnp.int32(0)}, device_id_type=MESH_ID)

        def relay_in(source, part):
            return pltpu.make_async_remote_copy(src_ref=in_ref.at[pl.ds(heavy_at + half + part * part_rows, part_rows)], dst_ref=relay_ref.at[pl.ds(part * part_rows, part_rows)], send_sem=relay_send.at[part], recv_sem=relay_recv.at[0, part], device_id={'fsdp': jnp.int32(source - 4)}, device_id_type=MESH_ID)

        def relay_out(source, part):
            return pltpu.make_async_remote_copy(src_ref=relay_ref.at[pl.ds(part * part_rows, part_rows)], dst_ref=out_ref.at[pl.ds(heavy_at + source * HEAVY_CAP + half + part * part_rows, part_rows)], send_sem=relay_send.at[part], recv_sem=relay_recv.at[source - 6, part], device_id={'fsdp': jnp.int32(0)}, device_id_type=MESH_ID)

        for source in (6, 7):
            @pl.when(my_dev == source)
            def _(source=source):
                for part in range(RELAY_PARTS):
                    relay_in(source, part).start()
        for source in range(1, n_dev):
            @pl.when(my_dev == source)
            def _(source=source):
                heavy_copy(source).start()
        for hop in range(1, n_dev):
            base_copy(hop).start()
        own = pltpu.make_async_copy(in_ref.at[pl.ds(0, BASE_CAP)], local.at[pl.ds(0, BASE_CAP)], local_sem.at[0])
        own.start()
        own.wait()
        back = pltpu.make_async_copy(local.at[pl.ds(0, BASE_CAP)], out_ref.at[pl.ds(0, BASE_CAP)], local_sem.at[0])
        back.start()

        @pl.when(my_dev == 0)
        def _():
            place = pl.ds(BASE_CAP, HEAVY_CAP)
            mine = pltpu.make_async_copy(in_ref.at[pl.ds(heavy_at, HEAVY_CAP)], local.at[place], local_sem.at[1])
            mine.start()
            mine.wait()
            mine = pltpu.make_async_copy(local.at[place], out_ref.at[pl.ds(heavy_at, HEAVY_CAP)], local_sem.at[1])
            mine.start()
            mine.wait()
        back.wait()
        for mid in (2, 3):
            @pl.when(my_dev == mid)
            def _(mid=mid):
                for part in range(RELAY_PARTS):
                    relay_in(mid + 4, part).wait_recv()
                    relay_out(mid + 4, part).start()
                for part in range(RELAY_PARTS):
                    relay_out(mid + 4, part).wait_send()
        for hop in range(1, n_dev):
            base_copy(hop).wait()
        for source in range(1, n_dev):
            @pl.when(my_dev == source)
            def _(source=source):
                heavy_copy(source).wait_send()
                if source >= 6:
                    for part in range(RELAY_PARTS):
                        relay_in(source, part).wait_send()

            @pl.when(my_dev == 0)
            def _(source=source):
                heavy_copy(source).wait_recv()
                if source >= 6:
                    for part in range(RELAY_PARTS):
                        relay_out(source, part).wait_recv()

    return pl.pallas_call(
        kernel,
        out_shape=(jax.ShapeDtypeStruct((n_rows, width), slot_grads.dtype), jax.ShapeDtypeStruct((half, width), slot_grads.dtype)),
        in_specs=[pl.BlockSpec(memory_space=pl.ANY)],
        out_specs=(pl.BlockSpec(memory_space=pl.ANY),) * 2,
        scratch_shapes=[
            pltpu.VMEM((BASE_CAP + HEAVY_CAP, width), slot_grads.dtype),
            pltpu.SemaphoreType.DMA((9,)),
            pltpu.SemaphoreType.DMA((15,)),
            pltpu.SemaphoreType.DMA((RELAY_PARTS,)),
            pltpu.SemaphoreType.DMA((2, RELAY_PARTS)),
            pltpu.SemaphoreType.DMA((2,)),
        ],
        compiler_params=pltpu.CompilerParams(collective_id=2, has_side_effects=True),
        cost_estimate=pl.CostEstimate(flops=10**9, bytes_accessed=10**8, transcendentals=0),
        name='return_rows',
    )(slot_grads)[0]


def write_table(rows, unique_ids, edges_at, starts, row_base, turn, vocab_dev, out_dtype, so_far=None):
    n_dev = starts.shape[0]
    list_len = unique_ids.shape[-1]
    width = rows.shape[-1]
    n_out = vocab_dev // OUT_ROWS
    step_blocks = STEP_ROWS // 8
    seg_blocks = OUT_ROWS // 8 + 1
    cap_blocks = -(-2 * n_dev * seg_blocks // step_blocks) * step_blocks

    def kernel(ids_s, edges_s, starts_s, info_s, rows_ref, *rest):
        old_ref = rest[0] if so_far is not None else None
        out_ref, staged, names_s, total, row_sem = rest[-5:]
        out_block = pl.program_id(0)
        base, turn_now = info_s[0], info_s[1]
        my_dev = base // vocab_dev
        cap = BASE_CAP + jnp.where(base == 0, HEAVY_CAP, 0)

        def spans(block):
            found = []
            for hop in range(n_dev):
                dest = my_dev ^ hop
                start = starts_s[dest] + turn_now * cap
                low = jnp.clip(edges_s[dest * (n_out + 1) + block] - start, 0, cap)
                high = jnp.clip(edges_s[dest * (n_out + 1) + block + 1] - start, 0, cap)
                for at, size, seg_row in ((0, BASE_CAP, hop * BASE_CAP), (BASE_CAP, HEAVY_CAP, n_dev * BASE_CAP + hop * HEAVY_CAP - BASE_CAP)):
                    first, last = jnp.clip(low, at, at + size), jnp.clip(high, at, at + size)
                    first_block = first // 8
                    count = jnp.where(last > first, (last + 7) // 8 - first_block, 0)
                    found.append((seg_row // 8 + first_block, count, dest * list_len + start + 8 * first_block))
            return found

        def start_fetch(block):
            slot = lax.rem(block, 2)
            where = jnp.int32(0)
            for row_block, count, name in spans(block):
                def one(i, at):
                    place = pl.ds(pl.multiple_of(8 * at, 8), 8)
                    pltpu.make_async_copy(rows_ref.at[pl.ds(pl.multiple_of(8 * (row_block + i), 8), 8)], staged.at[slot, place], row_sem.at[slot]).start()
                    names_s[slot, at] = name + 8 * i
                    return at + 1
                where = lax.fori_loop(0, count, one, where)
            names_s[slot, cap_blocks] = where

        @pl.when(out_block == 0)
        def _():
            start_fetch(out_block)

        @pl.when(out_block + 1 < n_out)
        def _():
            start_fetch(out_block + 1)

        slot = lax.rem(out_block, 2)
        n_blocks = names_s[slot, cap_blocks]

        def wait_one(i, carry):
            pltpu.make_async_copy(staged.at[slot, pl.ds(0, 8)], staged.at[slot, pl.ds(0, 8)], row_sem.at[slot]).wait()
            return carry

        lax.fori_loop(0, n_blocks, wait_one, 0)
        if so_far is None:
            total[...] = jnp.zeros_like(total)
        else:
            total[...] = old_ref[...]
        low_row = base + out_block * OUT_ROWS

        def add_step(step, carry):
            lane = lax.broadcasted_iota(jnp.int32, (8, STEP_ROWS), 1)
            wanted = jnp.full((8, STEP_ROWS), -1, jnp.int32)
            for block in range(step_blocks):
                at = step * step_blocks + block
                name = names_s[slot, jnp.minimum(at, n_blocks - 1)]
                for i in range(8):
                    row_id = ids_s[jnp.minimum(name + i, n_dev * list_len - 1)] - low_row
                    wanted = jnp.where(lane == 8 * block + i, jnp.where(at < n_blocks, row_id, -1), wanted)
            wanted = jnp.concatenate([wanted] * (OUT_ROWS // 8), axis=0)
            chooser = (wanted == lax.broadcasted_iota(jnp.int32, (OUT_ROWS, STEP_ROWS), 0)).astype(jnp.float32).astype(jnp.bfloat16)
            place = pl.ds(pl.multiple_of(step * STEP_ROWS, STEP_ROWS), STEP_ROWS)
            live = step * STEP_ROWS + lax.broadcasted_iota(jnp.int32, (STEP_ROWS, 1), 0) < 8 * n_blocks
            for col in range(0, width, 512):
                part = jnp.where(live, staged[slot, place, col:col + 512], 0.0)
                high = part.astype(jnp.bfloat16)
                rest_f32 = part - high.astype(jnp.float32)
                mid = rest_f32.astype(jnp.bfloat16)
                low = (rest_f32 - mid.astype(jnp.float32)).astype(jnp.bfloat16)
                acc = total[:, col:col + 512]
                for piece in (high, mid, low):
                    acc = acc + jnp.dot(chooser, piece, preferred_element_type=jnp.float32)
                total[:, col:col + 512] = acc
            return carry

        lax.fori_loop(0, (n_blocks + step_blocks - 1) // step_blocks, add_step, 0)
        out_ref[...] = total[...].astype(out_ref.dtype)

    tile = pl.BlockSpec((OUT_ROWS, width), lambda i, *_: (i, 0))
    extra = () if so_far is None else (so_far,)
    return pl.pallas_call(
        kernel,
        out_shape=jax.ShapeDtypeStruct((vocab_dev, width), out_dtype),
        grid_spec=pltpu.PrefetchScalarGridSpec(
            num_scalar_prefetch=4,
            grid=(n_out,),
            in_specs=[pl.BlockSpec(memory_space=pl.ANY)] + [tile] * len(extra),
            out_specs=tile,
            scratch_shapes=[
                pltpu.VMEM((2, 8 * cap_blocks, width), jnp.float32),
                pltpu.SMEM((2, cap_blocks + 1), jnp.int32),
                pltpu.VMEM((OUT_ROWS, width), jnp.float32),
                pltpu.SemaphoreType.DMA((2,)),
            ],
        ),
        compiler_params=pltpu.CompilerParams(vmem_limit_bytes=56 * 1024 * 1024),
        cost_estimate=pl.CostEstimate(flops=4 * 10**9, bytes_accessed=2 * 10**8, transcendentals=0),
        name='write_table',
    )(unique_ids.reshape(-1), edges_at.reshape(-1), starts, jnp.stack([row_base, turn]).astype(jnp.int32), rows, *extra)


def norm_back(rows_f32, d_normed, gain_vec):
    inv_rms = lax.rsqrt(jnp.mean(rows_f32 * rows_f32, axis=-1, keepdims=True) + RMS_EPS)
    scaled = d_normed * gain_vec
    along = jnp.mean(scaled * rows_f32, axis=-1, keepdims=True) * (inv_rms * inv_rms * inv_rms)
    return scaled * inv_rms - rows_f32 * along


def solution(mesh):
    tok_spec = P(('dp', 'fsdp'), None)
    seq_spec = P(('dp', 'fsdp'), None, None)
    part_vec = P(('dp', 'fsdp'))
    vec_spec = P('fsdp')
    mat_spec = P('fsdp', None)

    def device_step(tok_ids, grad_out, emb_table, norm_gain, w_query, w_kv_down, kv_gain, w_kv_up, w_out):
        seq_count, seq_len = tok_ids.shape
        vocab_dev, d_model = emb_table.shape
        tok_count = seq_count * seq_len
        n_dev = mesh.shape['fsdp']
        my_dev = lax.axis_index('fsdp')
        row_base = my_dev * vocab_dev
        n_slots = n_dev * BASE_CAP + HEAVY_CAP
        owner, owner_rank, unique_ids, counts = plan_ids(tok_ids.reshape(tok_count), vocab_dev, n_dev)
        notes = lax.all_gather(jnp.concatenate([unique_ids, counts, jnp.zeros((-(tok_count + n_dev) % 128,), jnp.int32)]), 'fsdp')
        all_unique, all_counts = notes[:, :tok_count], notes[:, tok_count:tok_count + n_dev]
        turns = jnp.max((all_counts + owner_cap(jnp.arange(n_dev)) - 1) // owner_cap(jnp.arange(n_dev)))
        is_me = jnp.arange(n_dev) == my_dev
        starts = jnp.sum(jnp.where(is_me[None, :], shifted_sum(all_counts), 0), axis=1)

        def slot_spread(turn):
            slot_of = slots_of(owner, owner_rank, my_dev, n_dev, turn)
            return (slot_of[:, None] == jnp.arange(n_slots)[None, :]).astype(jnp.bfloat16)

        def fetch_turn(turn):
            turn_starts = starts + turn * owner_cap(my_dev)
            slot_rows = swap_rows(pick_rows(emb_table, all_unique, turn_starts, row_base, n_dev), n_dev)
            return slot_rows, jnp.dot(slot_spread(turn), slot_rows, preferred_element_type=jnp.float32).astype(jnp.bfloat16)

        slot_rows, tok_rows = fetch_turn(0)
        tok_rows = lax.fori_loop(1, turns, lambda turn, have: have + fetch_turn(turn)[1], tok_rows)
        full_weights = tuple(lax.all_gather(shard_piece, 'fsdp', tiled=True) for shard_piece in (norm_gain, w_query, w_kv_down, kv_gain, w_kv_up, w_out))
        gain_f32 = full_weights[0].astype(jnp.float32)
        grad_rows = grad_out.reshape(tok_count, d_model)
        block_out, d_normed, weight_grads = block_step(tok_rows, grad_rows, full_weights, seq_count)
        toks_f32 = tok_rows.astype(jnp.float32)
        d_gain = jnp.sum(d_normed.astype(jnp.float32) * toks_f32 * lax.rsqrt(jnp.mean(toks_f32 * toks_f32, axis=-1, keepdims=True) + RMS_EPS), axis=0)
        edges = row_base + OUT_ROWS * jnp.arange(vocab_dev // OUT_ROWS + 1)
        edges_at = jnp.sum(((all_unique[:, None, :] >= 0) & (all_unique[:, None, :] < edges[None, :, None])).astype(jnp.int32), axis=-1)

        def one_turn(dy_rows, dn_rows):
            spread = slot_spread(0)
            slot_dy = lax.dot_general(spread, dy_rows, ROW_DIMS, preferred_element_type=jnp.float32)
            slot_dn = lax.dot_general(spread, dn_rows, ROW_DIMS, preferred_element_type=jnp.float32)
            slot_grads = slot_dy + norm_back(slot_rows.astype(jnp.float32), slot_dn, gain_f32)
            return write_table(return_rows(slot_grads, n_dev), all_unique, edges_at, starts, row_base, jnp.int32(0), vocab_dev, jnp.bfloat16)

        def many_turns(dy_rows, dn_rows):
            d_rows = dy_rows.astype(jnp.float32) + norm_back(toks_f32, dn_rows.astype(jnp.float32), gain_f32)

            def add_turn(turn, table):
                slot_grads = lax.dot_general(slot_spread(turn).astype(jnp.float32), d_rows, ROW_DIMS, precision=lax.Precision.HIGHEST, preferred_element_type=jnp.float32)
                return write_table(return_rows(slot_grads, n_dev), all_unique, edges_at, starts, row_base, turn, vocab_dev, jnp.float32, table)

            return lax.fori_loop(0, turns, add_turn, jnp.zeros((vocab_dev, d_model), jnp.float32)).astype(jnp.bfloat16)

        grad_table = lax.cond(turns > 1, many_turns, one_turn, grad_rows, d_normed)
        grad_shards = tuple(lax.psum_scatter(full_grad, 'fsdp', scatter_dimension=0, tiled=True) for full_grad in (d_gain,) + weight_grads)
        return (block_out.reshape(seq_count, seq_len, d_model), grad_table) + grad_shards

    return jax.shard_map(device_step, mesh=mesh, in_specs=(tok_spec, seq_spec, mat_spec, vec_spec, mat_spec, mat_spec, vec_spec, mat_spec, mat_spec), out_specs=(seq_spec, tok_spec, part_vec, tok_spec, tok_spec, part_vec, tok_spec, tok_spec), check_vma=False)
```

```python
import math
import jax
import jax.numpy as jnp
from jax import lax
from jax.experimental import pallas as pl
from jax.experimental.pallas import tpu as pltpu
from jax.sharding import PartitionSpec as P

ALL, NEW = ..., None
ROW, COL, LAST = 0, 1, -1
TILE_ROWS, LANES, PAIR = 8, 128, 2
SMALL_FLOPS, LARGE_FLOPS, SOME_BYTES = 4 * 10**9, 2 * 10**10, 10**8
MUCH_VMEM, MOST_VMEM = 48 * 2**20, 60 * 2**20
NOPE_DIM = 128
ROPE_DIM = 64
VALUE_DIM = 128
ROPE_THETA = 50000.0
RMS_EPS = 1e-6
ATTN_SCALE = (NOPE_DIM + ROPE_DIM) ** -0.5 * (0.1 * math.log(32.0) + 1.0) ** 2
LOG2_E = math.log2(math.e)
ROW_DIMS = (((0,), (0,)), ((), ()))
COL_DIMS = (((1,), (1,)), ((), ()))
PAIR_DIM = 2 * (NOPE_DIM + ROPE_DIM)
HALF_ROPE = ROPE_DIM // 2
Q_ROWS = 256


def cost_of(flops):
    return pl.CostEstimate(flops=flops, bytes_accessed=SOME_BYTES, transcendentals=0)


def row_iota(shape):
    return lax.broadcasted_iota(jnp.int32, shape, ROW)


def col_iota(shape):
    return lax.broadcasted_iota(jnp.int32, shape, COL)


def rms_scale(in_vals, gain_vec):
    vals_f32 = in_vals.astype(jnp.float32)
    inv_rms = lax.rsqrt(jnp.mean(vals_f32 * vals_f32, axis=LAST, keepdims=True) + RMS_EPS)
    return (vals_f32 * inv_rms * gain_vec).astype(jnp.bfloat16)


def norm_back(rows_f32, d_normed, gain_vec):
    inv_rms = lax.rsqrt(jnp.mean(rows_f32 * rows_f32, axis=LAST, keepdims=True) + RMS_EPS)
    scaled = d_normed * gain_vec
    along = jnp.mean(scaled * rows_f32, axis=LAST, keepdims=True) * (inv_rms * inv_rms * inv_rms)
    return scaled * inv_rms - rows_f32 * along


def gain_back(rows_f32, d_normed):
    inv_rms = lax.rsqrt(jnp.mean(rows_f32 * rows_f32, axis=LAST, keepdims=True) + RMS_EPS)
    return jnp.sum(d_normed * (rows_f32 * inv_rms), axis=ROW)


def pair_source(width):
    at = jnp.arange(width)
    turned = at - 2 * NOPE_DIM
    part, head, i = turned // (2 * HALF_ROPE), lax.rem(turned // HALF_ROPE, PAIR), lax.rem(turned, HALF_ROPE)
    plain = (NOPE_DIM + ROPE_DIM) * (at // NOPE_DIM) + lax.rem(at, NOPE_DIM)
    return jnp.where(at < 2 * NOPE_DIM, plain, (NOPE_DIM + ROPE_DIM) * head + NOPE_DIM + HALF_ROPE * part + i)


def arrange_weights(w_query, w_down):
    rows, query_dim = w_query.shape
    kv_rank = w_down.shape[COL] - ROPE_DIM
    down_dim = kv_rank + 2 * ROPE_DIM
    pair_pick = (jnp.arange(PAIR_DIM)[:, NEW] == pair_source(PAIR_DIM)[NEW, :]).astype(w_query.dtype)
    twice = HALF_ROPE * (jnp.arange(2 * ROPE_DIM) // (2 * HALF_ROPE)) + lax.rem(jnp.arange(2 * ROPE_DIM), HALF_ROPE)
    twice_pick = (jnp.arange(ROPE_DIM)[:, NEW] == twice[NEW, :]).astype(w_query.dtype)

    def kernel(query_ref, down_ref, pair_ref, twice_ref, out_ref, low_ref):
        for at in range(0, query_dim, PAIR_DIM):
            out_ref[:, at:at + PAIR_DIM] = jnp.dot(query_ref[:, at:at + PAIR_DIM], pair_ref[ALL], preferred_element_type=jnp.float32).astype(out_ref.dtype)
        low_ref[:, :kv_rank] = down_ref[:, :kv_rank]
        low_ref[:, kv_rank:] = jnp.dot(down_ref[:, kv_rank:], twice_ref[ALL], preferred_element_type=jnp.float32).astype(low_ref.dtype)

    return pl.pallas_call(
        kernel,
        out_shape=(jax.ShapeDtypeStruct((rows, query_dim), w_query.dtype), jax.ShapeDtypeStruct((rows, down_dim), w_query.dtype)),
        in_specs=[pl.BlockSpec(memory_space=pltpu.VMEM)] * 4,
        out_specs=(pl.BlockSpec(memory_space=pltpu.VMEM),) * 2,
        cost_estimate=cost_of(SMALL_FLOPS),
        name='arrange_weights',
    )(w_query, w_down, pair_pick, twice_pick)


def head_columns(d_query_w):
    rows = d_query_w.shape[ROW]
    pairs = d_query_w.reshape(rows, -1, PAIR_DIM)
    plain = pairs[ALL, :2 * NOPE_DIM].reshape(rows, -1, 2, NOPE_DIM)
    rotary = pairs[ALL, 2 * NOPE_DIM:].reshape(rows, -1, 2, 2, HALF_ROPE)
    rotary = jnp.swapaxes(rotary, 2, 3).reshape(rows, -1, 2, ROPE_DIM)
    return jnp.concatenate([plain, rotary], axis=LAST).reshape(rows, -1)


def rope_tables(seq_len):
    positions = jnp.arange(seq_len, dtype=jnp.float32)
    inv_freq = ROPE_THETA ** (-2.0 * jnp.arange(HALF_ROPE, dtype=jnp.float32) / ROPE_DIM)
    rot_angle = positions[:, NEW] * inv_freq[NEW, :]
    cos_tab, sin_tab = jnp.cos(rot_angle), jnp.sin(rot_angle)
    return jnp.concatenate([cos_tab] * 4, axis=COL), jnp.concatenate([-sin_tab, -sin_tab, sin_tab, sin_tab], axis=COL)


def attend_pairs(q_all, kv_all, pe_all, d_mix, seq_count, side):
    tok_count = q_all.shape[ROW]
    seq_len = tok_count // seq_count
    n_pairs = q_all.shape[COL] // PAIR_DIM
    kv_dim = NOPE_DIM + VALUE_DIM
    cos_tab, sin_tab = rope_tables(seq_len)

    def kernel(side_s, q_ref, kv_ref, pe_ref, do_ref, cos_ref, sin_ref, mix_ref, own_ref, give_ref, dq_ref, dkv_ref, dpe_ref, key_acc):
        pair = pl.program_id(1)
        cos_vals, sin_vals = cos_ref[ALL], sin_ref[ALL]
        lane = col_iota((seq_len, 2 * ROPE_DIM))

        def turn(vals):
            return vals * cos_vals + pltpu.roll(vals, ROPE_DIM, 1) * sin_vals

        def turn_back(vals):
            return vals * cos_vals - pltpu.roll(vals, ROPE_DIM, 1) * sin_vals

        k_rot = turn(pe_ref[ALL].astype(jnp.float32)).astype(jnp.bfloat16)
        q_rot = turn(q_ref[:, 2 * NOPE_DIM:].astype(jnp.float32)).astype(jnp.bfloat16)
        n_blocks = seq_len // Q_ROWS
        d_q_rot = [None] * n_blocks
        d_k_rot = jnp.zeros((seq_len, 2 * ROPE_DIM), jnp.float32)
        in_head = [lax.rem(lane // HALF_ROPE, PAIR) == head for head in range(2)]
        keys = [jnp.concatenate([kv_ref[:, kv_dim * head:kv_dim * head + NOPE_DIM], jnp.where(in_head[head], k_rot, jnp.zeros_like(k_rot))], axis=COL) for head in range(2)]
        values = [kv_ref[:, kv_dim * head + NOPE_DIM:kv_dim * (head + 1)] for head in range(2)]
        queries = [jnp.concatenate([q_ref[:, NOPE_DIM * head:NOPE_DIM * (head + 1)], q_rot], axis=COL) for head in range(2)]
        d_out = [do_ref[:, VALUE_DIM * head:VALUE_DIM * (head + 1)] for head in range(2)]
        d_keys, d_values = {}, {}
        chains = [(head, block) for head in range(2) for block in range(n_blocks)]

        def first_dots(chain):
            head, block = chain
            rows, upto = slice(block * Q_ROWS, (block + 1) * Q_ROWS), (block + 1) * Q_ROWS
            scores = lax.dot_general(queries[head][rows], keys[head][:upto], COL_DIMS, preferred_element_type=jnp.float32)
            return scores, lax.dot_general(d_out[head][rows], values[head][:upto], COL_DIMS, preferred_element_type=jnp.float32)

        def softmax(chain, scores):
            _, block = chain
            row_at = block * Q_ROWS + row_iota(scores.shape)
            col_at = col_iota(scores.shape)
            scores = jnp.where(row_at >= col_at, scores, -1e30)
            powers = jnp.exp2((scores - jnp.max(scores, axis=LAST, keepdims=True)) * (ATTN_SCALE * LOG2_E))
            return powers * (1.0 / jnp.sum(powers, axis=LAST, keepdims=True))

        def last_dots(chain, probs, d_probs):
            head, block = chain
            rows, upto = slice(block * Q_ROWS, (block + 1) * Q_ROWS), (block + 1) * Q_ROWS
            probs_low = probs.astype(jnp.bfloat16)
            mixed = jnp.dot(probs_low, values[head][:upto], preferred_element_type=jnp.float32)
            mix_ref[rows, VALUE_DIM * head:VALUE_DIM * (head + 1)] = mixed.astype(jnp.bfloat16)
            leaning = jnp.sum(mixed * d_out[head][rows].astype(jnp.float32), axis=LAST, keepdims=True)
            d_scores = (probs * (d_probs - leaning)).astype(jnp.bfloat16)
            d_queries = jnp.dot(d_scores, keys[head][:upto], preferred_element_type=jnp.float32) * ATTN_SCALE
            dq_ref[rows, NOPE_DIM * head:NOPE_DIM * (head + 1)] = d_queries[:, :NOPE_DIM].astype(jnp.bfloat16)
            d_q_rot[block] = d_queries[:, NOPE_DIM:] if d_q_rot[block] is None else d_q_rot[block] + d_queries[:, NOPE_DIM:]
            key_part = lax.dot_general(d_scores, queries[head][rows], ROW_DIMS, preferred_element_type=jnp.float32)
            value_part = lax.dot_general(probs_low, d_out[head][rows], ROW_DIMS, preferred_element_type=jnp.float32)
            for below in range(block + 1):
                cut = slice(below * Q_ROWS, (below + 1) * Q_ROWS)
                for have, part in ((d_keys, key_part), (d_values, value_part)):
                    have[head, below] = have[head, below] + part[cut] if (head, below) in have else part[cut]

        ready = first_dots(chains[0])
        held = None
        for at, chain in enumerate(chains):
            scores, d_probs = ready
            if at + 1 < len(chains):
                ready = first_dots(chains[at + 1])
            if held is not None:
                last_dots(*held)
            held = (chain, softmax(chain, scores), d_probs)
        last_dots(*held)
        for head in range(2):
            all_keys = jnp.concatenate([d_keys[head, below] for below in range(n_blocks)], axis=ROW) * ATTN_SCALE
            dkv_ref[:, kv_dim * head:kv_dim * head + NOPE_DIM] = all_keys[:, :NOPE_DIM].astype(jnp.bfloat16)
            dkv_ref[:, kv_dim * head + NOPE_DIM:kv_dim * (head + 1)] = jnp.concatenate([d_values[head, below] for below in range(n_blocks)], axis=ROW).astype(jnp.bfloat16)
            d_k_rot = d_k_rot + jnp.where(in_head[head], all_keys[:, NOPE_DIM:], 0.0)
        dq_ref[:, 2 * NOPE_DIM:] = turn_back(jnp.concatenate(d_q_rot, axis=ROW)).astype(jnp.bfloat16)

        is_own = lax.rem(pair, PAIR) == side_s[0]

        @pl.when(is_own)
        def _():
            own_ref[ALL] = mix_ref[ALL]

        @pl.when(jnp.logical_not(is_own))
        def _():
            give_ref[ALL] = mix_ref[ALL]

        @pl.when(pair == 0)
        def _():
            key_acc[ALL] = d_k_rot

        @pl.when(pair > 0)
        def _():
            key_acc[ALL] += d_k_rot

        @pl.when(pair == n_pairs - 1)
        def _():
            both = key_acc[ALL]
            both = both + pltpu.roll(both, 2 * ROPE_DIM - HALF_ROPE, 1)
            both = jnp.where(lax.rem(lane // HALF_ROPE, PAIR) == 0, turn_back(both), 0.0)
            dpe_ref[ALL] = both.astype(jnp.bfloat16)

    def pair_block(width):
        return pl.BlockSpec((seq_len, width), lambda seq, pair, side: (seq, pair))

    half_block = pl.BlockSpec((seq_len, 2 * VALUE_DIM), lambda seq, pair, side: (seq, pair // 2))
    seq_block = pl.BlockSpec((seq_len, 2 * ROPE_DIM), lambda seq, pair, side: (seq, 0))
    tab_block = pl.BlockSpec((seq_len, 2 * ROPE_DIM), lambda seq, pair, side: (0, 0))
    shape = lambda width: jax.ShapeDtypeStruct((tok_count, width), jnp.bfloat16)
    return pl.pallas_call(
        kernel,
        grid_spec=pltpu.PrefetchScalarGridSpec(
            num_scalar_prefetch=1,
            grid=(seq_count, n_pairs),
            in_specs=[pair_block(PAIR_DIM), pair_block(2 * kv_dim), seq_block, pair_block(2 * VALUE_DIM), tab_block, tab_block],
            out_specs=(pair_block(2 * VALUE_DIM), half_block, half_block, pair_block(PAIR_DIM), pair_block(2 * kv_dim), seq_block),
            scratch_shapes=[pltpu.VMEM((seq_len, 2 * ROPE_DIM), jnp.float32)],
        ),
        out_shape=(shape(n_pairs * 2 * VALUE_DIM), shape(n_pairs * VALUE_DIM), shape(n_pairs * VALUE_DIM), shape(n_pairs * PAIR_DIM), shape(n_pairs * 2 * kv_dim), shape(2 * ROPE_DIM)),
        compiler_params=pltpu.CompilerParams(vmem_limit_bytes=MUCH_VMEM),
        cost_estimate=cost_of(LARGE_FLOPS),
        name='attend_pairs',
    )(side.reshape(1), q_all, kv_all, pe_all, d_mix, cos_tab, sin_tab)


BASE_CAP = 144
HEAVY_CAP = 480
RELAY_ROWS = 240
RELAY_PARTS = 3
DEST_ROWS = BASE_CAP + HEAVY_CAP
GROUP_ROWS = 48
FETCH_SLOTS = 6
TABLE_SLOTS = 4
SLOT_TILE = 136
MIX_TILE = 256
OUT_ROWS = 128
STEP_ROWS = 128
MESH_ID = pl.DeviceIdType.MESH


def shifted_sum(counts):
    size = counts.shape[LAST]
    lower = jnp.arange(size)[:, NEW] < jnp.arange(size)[NEW, :]
    return jnp.sum(jnp.where(lower, counts[ALL, :, None], 0), axis=-2)


def owner_cap(owner):
    return BASE_CAP + jnp.where(owner == 0, HEAVY_CAP, 0)


def plan_ids(flat_ids, vocab_dev, n_dev):
    order = jnp.arange(flat_ids.shape[ROW])
    same_before = (flat_ids[:, NEW] == flat_ids[NEW, :]) & (order[:, NEW] < order[NEW, :])
    is_first = jnp.logical_not(jnp.any(same_before, axis=ROW))
    lower = (flat_ids[:, NEW] < flat_ids[NEW, :]) & is_first[:, NEW]
    unique_rank = jnp.sum(lower.astype(jnp.int32), axis=ROW)
    owner = flat_ids // vocab_dev
    owned = owner[:, NEW] == jnp.arange(n_dev)[NEW, :]
    counts = jnp.sum((owned & is_first[:, NEW]).astype(jnp.int32), axis=ROW)
    owner_rank = unique_rank - jnp.sum(jnp.where(owned, shifted_sum(counts)[NEW, :], 0), axis=COL)
    return owner, owner_rank, is_first, counts


def slots_of(owner, owner_rank, dev, n_dev, turn):
    cap = owner_cap(owner)
    within = owner_rank - turn * cap
    slot = jnp.where(within < BASE_CAP, BASE_CAP * (owner ^ dev) + within, BASE_CAP * (n_dev - 1) + within)
    return jnp.where((within >= 0) & (within < cap), slot, -1)


def slot_list(flat_ids, slot_of, is_first, n_slots):
    hits = (slot_of[:, NEW] == jnp.arange(n_slots)[NEW, :]) & is_first[:, NEW]
    return jnp.sum(jnp.where(hits, flat_ids[:, NEW] + 1, 0), axis=ROW) - 1


def wanted_lists(all_slots, my_dev, n_dev):
    hop = jnp.arange(n_dev)[:, NEW] ^ my_dev
    base = all_slots[:, :n_dev * BASE_CAP].reshape(n_dev, n_dev, BASE_CAP)
    base = jnp.sum(jnp.where((hop == jnp.arange(n_dev)[NEW, :])[:, :, NEW], base, 0), axis=COL)
    heavy = jnp.where(my_dev == 0, all_slots[:, n_dev * BASE_CAP:], -1)
    by_dest = jnp.concatenate([base, heavy], axis=COL)
    return jnp.sum(jnp.where((hop == jnp.arange(n_dev)[NEW, :])[:, :, NEW], by_dest[:, NEW, :], 0), axis=ROW)


def pick_rows(table, lists, my_dev):
    vocab_dev, width = table.shape
    n_dev = lists.shape[ROW]
    flat = lists.reshape(-1)
    at = jnp.arange(n_dev * DEST_ROWS)
    local = jnp.where(flat < 0, lax.rem(TILE_ROWS * at, vocab_dev), jnp.clip(flat - my_dev * vocab_dev, 0, vocab_dev - 1))
    tiles = TILE_ROWS * (local // TILE_ROWS)
    tags = lax.rem(local, TILE_ROWS) + TILE_ROWS * lax.rem(at, GROUP_ROWS)
    tags = jnp.broadcast_to(tags[:, NEW], (n_dev * DEST_ROWS, LANES))
    all_groups = DEST_ROWS // GROUP_ROWS
    few_groups = -(-BASE_CAP // GROUP_ROWS)

    def kernel(tiles_s, dev_s, table_ref, tags_ref, out_ref, fetched, named, picked, fetch_sem, name_sem, out_sem):
        per_dest = jnp.where(dev_s[0] == 0, all_groups, few_groups)
        n_groups = n_dev * per_dest

        def row_at(group):
            dest = group // per_dest
            return pl.multiple_of(dest * DEST_ROWS + GROUP_ROWS * (group - dest * per_dest), GROUP_ROWS)

        def start_fetch(group):
            slot = lax.rem(group, FETCH_SLOTS)
            row = row_at(jnp.minimum(group, n_groups - 1))
            pltpu.make_async_copy(tags_ref.at[pl.ds(row, GROUP_ROWS)], named.at[slot], name_sem.at[slot]).start()
            for i in range(GROUP_ROWS):
                pltpu.make_async_copy(table_ref.at[pl.ds(pl.multiple_of(tiles_s[row + i], TILE_ROWS), TILE_ROWS)], fetched.at[slot, pl.ds(TILE_ROWS * i, TILE_ROWS)], fetch_sem.at[slot]).start()

        def wait_fetch(slot):
            pltpu.make_async_copy(named.at[slot], named.at[slot], name_sem.at[slot]).wait()
            pltpu.make_async_copy(fetched.at[slot], fetched.at[slot], fetch_sem.at[slot]).wait()

        def out_copy(group):
            slot = lax.rem(group, TABLE_SLOTS)
            return pltpu.make_async_copy(picked.at[slot], out_ref.at[pl.ds(row_at(group), GROUP_ROWS)], out_sem.at[slot])

        for ahead in range(FETCH_SLOTS - 1):
            start_fetch(jnp.int32(ahead))

        def body(group, carry):
            @pl.when(group >= TABLE_SLOTS)
            def _():
                out_copy(group - TABLE_SLOTS).wait()

            slot = lax.rem(group, FETCH_SLOTS)
            wait_fetch(slot)
            start_fetch(group + FETCH_SLOTS - 1)
            lane = col_iota((GROUP_ROWS, LANES))
            name = named[slot]
            chooser = jnp.concatenate([(name == lane + at).astype(jnp.float32) for at in range(0, TILE_ROWS * GROUP_ROWS, LANES)], axis=COL).astype(jnp.bfloat16)
            picked[lax.rem(group, TABLE_SLOTS)] = jnp.dot(chooser, fetched[slot], preferred_element_type=jnp.float32).astype(jnp.bfloat16)
            out_copy(group).start()
            return carry

        lax.fori_loop(0, n_groups, body, 0)
        for ahead in range(FETCH_SLOTS - 1):
            wait_fetch(lax.rem(n_groups + ahead, FETCH_SLOTS))
        for back in range(TABLE_SLOTS, 0, -1):
            out_copy(n_groups - back).wait()

    return pl.pallas_call(
        kernel,
        out_shape=jax.ShapeDtypeStruct((n_dev * DEST_ROWS, width), table.dtype),
        grid_spec=pltpu.PrefetchScalarGridSpec(
            num_scalar_prefetch=2,
            grid=(1,),
            in_specs=[pl.BlockSpec(memory_space=pl.ANY)] * 2,
            out_specs=pl.BlockSpec(memory_space=pl.ANY),
            scratch_shapes=[
                pltpu.VMEM((FETCH_SLOTS, TILE_ROWS * GROUP_ROWS, width), table.dtype),
                pltpu.VMEM((FETCH_SLOTS, GROUP_ROWS, LANES), jnp.int32),
                pltpu.VMEM((TABLE_SLOTS, GROUP_ROWS, width), table.dtype),
                pltpu.SemaphoreType.DMA((FETCH_SLOTS,)),
                pltpu.SemaphoreType.DMA((FETCH_SLOTS,)),
                pltpu.SemaphoreType.DMA((TABLE_SLOTS,)),
            ],
        ),
        cost_estimate=cost_of(SMALL_FLOPS),
        name='pick_rows',
    )(tiles, my_dev.reshape(1), table, tags)


def greet_all(my_dev, n_dev):
    barrier = pltpu.get_barrier_semaphore()
    for hop in range(1, n_dev):
        pl.semaphore_signal(barrier, inc=1, device_id={'fsdp': my_dev ^ hop}, device_id_type=MESH_ID)
    pl.semaphore_wait(barrier, n_dev - 1)


def remote(source, target, send_sem, recv_sem, dest):
    return pltpu.make_async_remote_copy(src_ref=source, dst_ref=target, send_sem=send_sem, recv_sem=recv_sem, device_id={'fsdp': dest}, device_id_type=MESH_ID)


def swap_rows(picked, n_dev, work=None):
    width = picked.shape[LAST]
    n_slots = n_dev * BASE_CAP + HEAVY_CAP
    n_tiles = n_slots // SLOT_TILE
    tok_count = 0 if work is None else work[1].shape[ROW]
    heavy_at = n_dev * BASE_CAP
    part_rows = RELAY_ROWS // RELAY_PARTS

    def kernel(*refs):
        if work is None:
            in_ref, out_ref, relay_ref, local, send_sem, recv_sem, relay_send, relay_recv, local_sem = refs
        else:
            in_ref, at_ref, dy_ref, w_out_ref, out_ref, relay_ref, sums_ref, mix_ref, local, send_sem, recv_sem, relay_send, relay_recv, local_sem, dy_vals, w_vals, sums, mixes, load_sem, store_sem = refs
        my_dev = lax.axis_index('fsdp')
        greet_all(my_dev, n_dev)

        def base_copy(hop):
            return remote(in_ref.at[pl.ds(hop * DEST_ROWS, BASE_CAP)], out_ref.at[pl.ds(hop * BASE_CAP, BASE_CAP)], send_sem.at[hop], recv_sem.at[hop], my_dev ^ hop)

        def heavy_copy(dest):
            rows = HEAVY_CAP - (RELAY_ROWS if dest >= 6 else 0)
            return remote(in_ref.at[pl.ds(dest * DEST_ROWS + BASE_CAP, rows)], out_ref.at[pl.ds(heavy_at, rows)], send_sem.at[7 + dest], recv_sem.at[8], jnp.int32(dest))

        def relay_in(dest, part):
            at = dest * DEST_ROWS + DEST_ROWS - RELAY_ROWS + part * part_rows
            return remote(in_ref.at[pl.ds(at, part_rows)], relay_ref.at[pl.ds(part * part_rows, part_rows)], relay_send.at[dest - 6, part], relay_recv.at[part], jnp.int32(dest - 2))

        def relay_out(dest, part):
            at = heavy_at + HEAVY_CAP - RELAY_ROWS + part * part_rows
            return remote(relay_ref.at[pl.ds(part * part_rows, part_rows)], out_ref.at[pl.ds(at, part_rows)], relay_send.at[0, part], relay_recv.at[part], jnp.int32(dest))

        @pl.when(my_dev == 0)
        def _():
            for part in range(RELAY_PARTS):
                for dest in (6, 7):
                    relay_in(dest, part).start()
            for dest in (6, 7, 2, 4, 3, 5, 1):
                heavy_copy(dest).start()

        for hop in (6, 7, 2, 4, 3, 5, 1):
            base_copy(hop).start()
        if work is not None:
            loads = (pltpu.make_async_copy(dy_ref, dy_vals, load_sem.at[0]), pltpu.make_async_copy(w_out_ref, w_vals, load_sem.at[1]))
            for load in loads:
                load.start()
        own = pltpu.make_async_copy(in_ref.at[pl.ds(0, DEST_ROWS)], local, local_sem.at[0])
        own.start()
        own.wait()
        back = pltpu.make_async_copy(local.at[pl.ds(0, BASE_CAP)], out_ref.at[pl.ds(0, BASE_CAP)], local_sem.at[1])
        back.start()

        @pl.when(my_dev == 0)
        def _():
            mine = pltpu.make_async_copy(local.at[pl.ds(BASE_CAP, HEAVY_CAP)], out_ref.at[pl.ds(heavy_at, HEAVY_CAP)], local_sem.at[2])
            mine.start()
            mine.wait()

        back.wait()
        if work is not None:
            def sums_copy(tile):
                return pltpu.make_async_copy(sums.at[lax.rem(tile, PAIR)], sums_ref.at[pl.ds(pl.multiple_of(tile * SLOT_TILE, TILE_ROWS), SLOT_TILE)], store_sem.at[lax.rem(tile, PAIR)])

            def mix_copy(tile):
                return pltpu.make_async_copy(mixes.at[lax.rem(tile, PAIR)], mix_ref.at[pl.ds(pl.multiple_of(tile * MIX_TILE, TILE_ROWS), MIX_TILE)], store_sem.at[2 + lax.rem(tile, PAIR)])

            def sum_tile(tile, carry):
                @pl.when(tile >= 2)
                def _():
                    sums_copy(tile - 2).wait()

                slot = tile * SLOT_TILE + row_iota((SLOT_TILE, tok_count))
                chooser = (slot == at_ref[ALL]).astype(jnp.float32).astype(jnp.bfloat16)
                sums[lax.rem(tile, PAIR)] = jnp.dot(chooser, dy_vals[ALL], preferred_element_type=jnp.float32)
                sums_copy(tile).start()
                return carry

            def mix_tile(tile, carry):
                @pl.when(tile >= 2)
                def _():
                    mix_copy(tile - 2).wait()

                rows = dy_vals[pl.ds(pl.multiple_of(tile * MIX_TILE, MIX_TILE), MIX_TILE)]
                mixes[lax.rem(tile, PAIR)] = lax.dot_general(rows, w_vals[ALL], COL_DIMS, preferred_element_type=jnp.float32).astype(jnp.bfloat16)
                mix_copy(tile).start()
                return carry

            loads[0].wait()
            lax.fori_loop(0, n_tiles, sum_tile, 0)
        for mid in (4, 5):
            @pl.when(my_dev == mid)
            def _(mid=mid):
                for part in range(RELAY_PARTS):
                    relay_in(mid + 2, part).wait_recv()
                    relay_out(mid + 2, part).start()
                for part in range(RELAY_PARTS):
                    relay_out(mid + 2, part).wait_send()
        if work is not None:
            loads[1].wait()
            lax.fori_loop(0, tok_count // MIX_TILE, mix_tile, 0)
            for back_at in (2, 1):
                sums_copy(jnp.int32(n_tiles - back_at)).wait()
                mix_copy(jnp.int32(tok_count // MIX_TILE - back_at)).wait()
        for hop in range(1, n_dev):
            base_copy(hop).wait()
        for dest in range(1, n_dev):
            @pl.when(my_dev == dest)
            def _(dest=dest):
                heavy_copy(dest).wait_recv()
                if dest >= 6:
                    for part in range(RELAY_PARTS):
                        relay_out(dest, part).wait_recv()

            @pl.when(my_dev == 0)
            def _(dest=dest):
                heavy_copy(dest).wait_send()
                if dest >= 6:
                    for part in range(RELAY_PARTS):
                        relay_in(dest, part).wait_send()

    any_spec = pl.BlockSpec(memory_space=pl.ANY)
    out_shape = [jax.ShapeDtypeStruct((n_slots, width), picked.dtype), jax.ShapeDtypeStruct((RELAY_ROWS, width), picked.dtype)]
    in_specs = [any_spec]
    scratch_shapes = [
        pltpu.VMEM((DEST_ROWS, width), picked.dtype),
        pltpu.SemaphoreType.DMA((15,)),
        pltpu.SemaphoreType.DMA((9,)),
        pltpu.SemaphoreType.DMA((2, RELAY_PARTS)),
        pltpu.SemaphoreType.DMA((RELAY_PARTS,)),
        pltpu.SemaphoreType.DMA((3,)),
    ]
    if work is not None:
        in_specs += [pl.BlockSpec(memory_space=pltpu.VMEM), any_spec, any_spec]
        out_shape += [jax.ShapeDtypeStruct((n_slots, width), jnp.float32), jax.ShapeDtypeStruct((tok_count, work[2].shape[ROW]), jnp.bfloat16)]
        scratch_shapes += [
            pltpu.VMEM(work[1].shape, work[1].dtype),
            pltpu.VMEM(work[2].shape, work[2].dtype),
            pltpu.VMEM((2, SLOT_TILE, width), jnp.float32),
            pltpu.VMEM((2, MIX_TILE, work[2].shape[ROW]), jnp.bfloat16),
            pltpu.SemaphoreType.DMA((2,)),
            pltpu.SemaphoreType.DMA((4,)),
        ]
    outs = pl.pallas_call(
        kernel,
        out_shape=tuple(out_shape),
        in_specs=in_specs,
        out_specs=(any_spec,) * len(out_shape),
        scratch_shapes=scratch_shapes,
        compiler_params=pltpu.CompilerParams(collective_id=1 if work is None else 3, has_side_effects=True, vmem_limit_bytes=MUCH_VMEM),
        cost_estimate=cost_of(LARGE_FLOPS),
        name='swap_rows',
    )(picked, *(work or ()))
    return outs[0] if work is None else (outs[0], outs[2], outs[3])


def table_parts(source):
    if source < 6:
        return ((0, BASE_CAP), (BASE_CAP, HEAVY_CAP))
    return ((0, BASE_CAP), (BASE_CAP, HEAVY_CAP - RELAY_ROWS), (DEST_ROWS - RELAY_ROWS, RELAY_ROWS))


def permute_rows(parts, n_dev):
    base, direct, relayed = parts[:n_dev], parts[n_dev], parts[n_dev + 1]
    heavy = jnp.concatenate([direct, relayed], axis=ROW)
    passed = lax.ppermute(relayed, 'fsdp', [(6, 2), (7, 3)])
    arrived = {0: [heavy]}
    for source in (6, 7):
        arrived[source] = [lax.ppermute(direct, 'fsdp', [(source, 0)])]
    for source in (2, 4, 3, 5, 1):
        arrived[source] = [lax.ppermute(heavy, 'fsdp', [(source, 0)])]
    for source in (6, 7):
        arrived[source].append(lax.ppermute(passed, 'fsdp', [(source - 4, 0)]))
    base = [base[0]] + [lax.ppermute(base[hop], 'fsdp', [(dev, dev ^ hop) for dev in range(n_dev)]) for hop in range(1, n_dev)]
    return [piece for source in range(n_dev) for piece in [base[source]] + arrived[source]]


def return_rows(slot_grads, n_dev):
    width = slot_grads.shape[LAST]
    heavy_at = n_dev * BASE_CAP

    def kernel(in_ref, out_ref, local, send_sem, recv_sem, local_sem):
        my_dev = lax.axis_index('fsdp')
        greet_all(my_dev, n_dev)

        def base_copy(hop):
            place = pl.ds(hop * BASE_CAP, BASE_CAP)
            return remote(in_ref.at[place], out_ref.at[place], send_sem.at[hop], recv_sem.at[hop], my_dev ^ hop)

        def heavy_copy(source):
            return remote(in_ref.at[pl.ds(heavy_at, HEAVY_CAP)], out_ref.at[pl.ds(heavy_at + source * HEAVY_CAP, HEAVY_CAP)], send_sem.at[8], recv_sem.at[7 + source], jnp.int32(0))

        for source in range(1, n_dev):
            @pl.when(my_dev == source)
            def _(source=source):
                heavy_copy(source).start()
        for hop in range(1, n_dev):
            base_copy(hop).start()

        def bounce(at, rows):
            for one in (pltpu.make_async_copy(in_ref.at[pl.ds(at, rows)], local.at[pl.ds(0, rows)], local_sem), pltpu.make_async_copy(local.at[pl.ds(0, rows)], out_ref.at[pl.ds(at, rows)], local_sem)):
                one.start()
                one.wait()

        bounce(0, BASE_CAP)

        @pl.when(my_dev == 0)
        def _():
            bounce(heavy_at, HEAVY_CAP)

        for hop in range(1, n_dev):
            base_copy(hop).wait()
        for source in range(1, n_dev):
            @pl.when(my_dev == source)
            def _(source=source):
                heavy_copy(source).wait_send()

            @pl.when(my_dev == 0)
            def _(source=source):
                heavy_copy(source).wait_recv()

    arrived = pl.pallas_call(
        kernel,
        out_shape=jax.ShapeDtypeStruct((n_dev * DEST_ROWS, width), slot_grads.dtype),
        in_specs=[pl.BlockSpec(memory_space=pl.ANY)],
        out_specs=pl.BlockSpec(memory_space=pl.ANY),
        scratch_shapes=[
            pltpu.VMEM((HEAVY_CAP, width), slot_grads.dtype),
            pltpu.SemaphoreType.DMA((9,)),
            pltpu.SemaphoreType.DMA((15,)),
            pltpu.SemaphoreType.DMA,
        ],
        compiler_params=pltpu.CompilerParams(collective_id=2, has_side_effects=True),
        cost_estimate=cost_of(SMALL_FLOPS),
        name='return_rows',
    )(slot_grads)
    pieces = []
    for source in range(n_dev):
        pieces.append(arrived[source * BASE_CAP:(source + 1) * BASE_CAP])
        heavy_part = arrived[heavy_at + source * HEAVY_CAP:heavy_at + (source + 1) * HEAVY_CAP]
        pieces += [heavy_part[start - BASE_CAP:start - BASE_CAP + rows] for start, rows in table_parts(source)[1:]]
    return pieces


def table_plan(lists, my_dev, vocab_dev):
    n_dev = lists.shape[ROW]
    n_out = vocab_dev // OUT_ROWS
    edges = my_dev * vocab_dev + OUT_ROWS * jnp.arange(n_out + 1)
    below = (lists[NEW, :, :] >= 0) & (lists[NEW, :, :] < edges[:, NEW, NEW])
    upto = jnp.sum(below.astype(jnp.int32), axis=LAST)
    low, high = upto[:-1], upto[1:]
    firsts = low // TILE_ROWS
    counts = jnp.where(high > low, (high + 7) // TILE_ROWS - firsts, 0)
    names = jnp.broadcast_to(lists.reshape(-1, 1), (n_dev * DEST_ROWS, LANES))
    return firsts.reshape(-1), counts.reshape(-1), names


def write_table(pieces, plan, my_dev, vocab_dev, out_dtype, so_far=None):
    firsts, counts, names = plan
    width = pieces[0].shape[LAST]
    n_out = vocab_dev // OUT_ROWS
    n_part = len(pieces)
    n_source = firsts.shape[ROW] // n_out
    tile_blocks = OUT_ROWS // TILE_ROWS
    cap_rows = TILE_ROWS * n_source * (tile_blocks + 1)
    cap_rows = -(-cap_rows // STEP_ROWS) * STEP_ROWS

    def kernel(firsts_s, counts_s, dev_s, *refs):
        part_refs, names_ref = refs[:n_part], refs[n_part]
        old_ref = refs[n_part + 1] if so_far is not None else None
        out_ref, staged, named, total, ready, filled_s, row_sem, out_sem, old_sem = refs[-9:]

        def start_fetch(block):
            slot = lax.rem(block, TABLE_SLOTS)
            where = jnp.int32(0)
            first_ref = 0
            for source in range(n_source):
                parts = table_parts(source)
                first = firsts_s[block * n_source + source]

                def one(i, at, parts=parts, source=source, first=first, first_ref=first_ref):
                    block_at = first + i
                    place = pl.ds(pl.multiple_of(TILE_ROWS * at, TILE_ROWS), TILE_ROWS)
                    named[slot, place] = names_ref[pl.ds(pl.multiple_of(source * DEST_ROWS + TILE_ROWS * block_at, TILE_ROWS), TILE_ROWS)]
                    for part, (start, rows) in enumerate(parts):
                        @pl.when((block_at >= start // TILE_ROWS) & (block_at < (start + rows) // TILE_ROWS))
                        def _(part=part, start=start):
                            pltpu.make_async_copy(part_refs[first_ref + part].at[pl.ds(pl.multiple_of(TILE_ROWS * block_at - start, TILE_ROWS), TILE_ROWS)], staged.at[slot, place], row_sem.at[slot]).start()
                    return at + 1

                where = lax.fori_loop(0, counts_s[block * n_source + source], one, where)
                first_ref += len(parts)
            filled_s[slot] = where

        def out_copy(block):
            slot = lax.rem(block, TABLE_SLOTS)
            return pltpu.make_async_copy(ready.at[slot], out_ref.at[pl.ds(pl.multiple_of(block * OUT_ROWS, OUT_ROWS), OUT_ROWS)], out_sem.at[slot])

        for ahead in range(TABLE_SLOTS - 1):
            start_fetch(jnp.int32(ahead))

        def body(out_block, carry):
            @pl.when(out_block + TABLE_SLOTS - 1 < n_out)
            def _():
                start_fetch(out_block + TABLE_SLOTS - 1)

            @pl.when(out_block >= TABLE_SLOTS)
            def _():
                out_copy(out_block - TABLE_SLOTS).wait()

            slot = lax.rem(out_block, TABLE_SLOTS)
            n_blocks = filled_s[slot]

            def wait_one(i, carry):
                pltpu.make_async_copy(staged.at[slot, pl.ds(0, TILE_ROWS)], staged.at[slot, pl.ds(0, TILE_ROWS)], row_sem.at[slot]).wait()
                return carry

            lax.fori_loop(0, n_blocks, wait_one, 0)
            low_row = dev_s[0] * vocab_dev + out_block * OUT_ROWS

            def summed(start, rows, store):
                place = pl.ds(start, rows)
                live = start + row_iota((rows, OUT_ROWS)) < TILE_ROWS * n_blocks
                lane = col_iota((rows, OUT_ROWS))
                chooser = ((named[slot, place] - low_row == lane) & live).astype(jnp.float32)
                chooser = jnp.concatenate([chooser] * 3, axis=ROW).T.astype(jnp.bfloat16)
                for col in range(0, width, 512):
                    part = jnp.where(live[:, :1], staged[slot, place, col:col + 512], 0.0)
                    high = part.astype(jnp.bfloat16)
                    left = part - high.astype(jnp.float32)
                    mid = left.astype(jnp.bfloat16)
                    low = (left - mid.astype(jnp.float32)).astype(jnp.bfloat16)
                    stacked = jnp.concatenate([high, mid, low], axis=ROW)
                    store(col, jnp.dot(chooser, stacked, preferred_element_type=jnp.float32))

            def store_out(col, vals):
                ready[slot, :, col:col + 512] = vals.astype(out_dtype)

            def store_more(col, vals):
                total[:, col:col + 512] += vals

            few = jnp.int32(-1) if so_far is not None else n_blocks

            @pl.when(few == 0)
            def _():
                ready[slot] = jnp.zeros((OUT_ROWS, width), out_dtype)

            @pl.when((few > 0) & (few <= STEP_ROWS // 16))
            def _():
                summed(0, STEP_ROWS // 2, store_out)

            @pl.when((few > STEP_ROWS // 16) & (few <= STEP_ROWS // TILE_ROWS))
            def _():
                summed(0, STEP_ROWS, store_out)

            @pl.when((few < 0) | (few > STEP_ROWS // TILE_ROWS))
            def _():
                if so_far is None:
                    total[ALL] = jnp.zeros_like(total)
                else:
                    old = pltpu.make_async_copy(old_ref.at[pl.ds(pl.multiple_of(out_block * OUT_ROWS, OUT_ROWS), OUT_ROWS)], total, old_sem)
                    old.start()
                    old.wait()

                def add_step(step, carry):
                    summed(pl.multiple_of(step * STEP_ROWS, STEP_ROWS), STEP_ROWS, store_more)
                    return carry

                lax.fori_loop(0, (TILE_ROWS * n_blocks + STEP_ROWS - 1) // STEP_ROWS, add_step, 0)
                ready[slot] = total[ALL].astype(out_dtype)

            out_copy(out_block).start()
            return carry

        lax.fori_loop(0, n_out, body, 0)
        for back in range(TABLE_SLOTS, 0, -1):
            out_copy(n_out - back).wait()

    extra = () if so_far is None else (so_far,)
    any_spec = pl.BlockSpec(memory_space=pl.ANY)
    return pl.pallas_call(
        kernel,
        out_shape=jax.ShapeDtypeStruct((vocab_dev, width), out_dtype),
        grid_spec=pltpu.PrefetchScalarGridSpec(
            num_scalar_prefetch=3,
            grid=(1,),
            in_specs=[any_spec] * n_part + [pl.BlockSpec(names.shape, lambda i, *_: (0, 0))] + [any_spec] * len(extra),
            out_specs=any_spec,
            scratch_shapes=[
                pltpu.VMEM((TABLE_SLOTS, cap_rows, width), jnp.float32),
                pltpu.VMEM((TABLE_SLOTS, cap_rows, LANES), jnp.int32),
                pltpu.VMEM((OUT_ROWS, width), jnp.float32),
                pltpu.VMEM((TABLE_SLOTS, OUT_ROWS, width), out_dtype),
                pltpu.SMEM((TABLE_SLOTS,), jnp.int32),
                pltpu.SemaphoreType.DMA((TABLE_SLOTS,)),
                pltpu.SemaphoreType.DMA((TABLE_SLOTS,)),
                pltpu.SemaphoreType.DMA,
            ],
        ),
        compiler_params=pltpu.CompilerParams(vmem_limit_bytes=MOST_VMEM),
        cost_estimate=cost_of(SMALL_FLOPS),
        name='write_table',
    )(firsts, counts, my_dev.reshape(1), *pieces, names, *extra)


GRAD_TILE = 512
NORM_ROWS = 256


def after(vals, *deps):
    return lax.optimization_barrier((vals,) + deps)[0]


def side_blocks(rows, side, n_dev):
    block = rows.shape[COL] // n_dev
    cuts = [rows[:, at * block:(at + 1) * block] for at in range(n_dev)]
    even, odd = jnp.concatenate(cuts[0::2], axis=COL), jnp.concatenate(cuts[1::2], axis=COL)
    return jnp.where(side == 0, even, odd), jnp.where(side == 0, odd, even)


def expand_rows(slot_of, slot_rows, gain_f32, side, n_dev):
    n_slots, width = slot_rows.shape
    tok_count = slot_of.shape[ROW]
    slot_cols = jnp.broadcast_to(slot_of[:, NEW], (tok_count, LANES))

    def kernel(side_s, at_ref, rows_ref, gain_ref, tok_ref, norm_ref, own_ref, give_ref):
        lane = col_iota((NORM_ROWS, n_slots))
        chooser = (at_ref[:, :1] == lane).astype(jnp.float32).astype(jnp.bfloat16)
        vals = jnp.dot(chooser, rows_ref[ALL], preferred_element_type=jnp.float32)
        tok_ref[ALL] = vals.astype(jnp.bfloat16)
        inv_rms = lax.rsqrt(jnp.mean(vals * vals, axis=LAST, keepdims=True) + RMS_EPS)
        normed = (vals * inv_rms * gain_ref[ALL]).astype(jnp.bfloat16)
        norm_ref[ALL] = normed
        own_ref[ALL], give_ref[ALL] = side_blocks(normed, side_s[0], n_dev)

    def row_block(cols):
        return pl.BlockSpec((NORM_ROWS, cols), lambda step, side: (step, 0))

    def whole(rows):
        return pl.BlockSpec((rows, width), lambda step, side: (0, 0))

    shape = lambda cols: jax.ShapeDtypeStruct((tok_count, cols), jnp.bfloat16)
    return pl.pallas_call(
        kernel,
        grid_spec=pltpu.PrefetchScalarGridSpec(
            num_scalar_prefetch=1,
            grid=(tok_count // NORM_ROWS,),
            in_specs=[row_block(128), whole(n_slots), whole(1)],
            out_specs=(row_block(width), row_block(width), row_block(width // 2), row_block(width // 2)),
        ),
        out_shape=(shape(width), shape(width), shape(width // 2), shape(width // 2)),
        compiler_params=pltpu.CompilerParams(vmem_limit_bytes=MUCH_VMEM),
        cost_estimate=cost_of(2 * tok_count * n_slots * width),
        name='expand_rows',
    )(side.reshape(1), slot_cols, slot_rows, gain_f32.reshape(1, width))


def grad_rows_of(left, right, tile=GRAD_TILE):
    tok_count, left_dim = left[0].shape
    n_cols = right[0].shape[COL]
    block = 256

    def kernel(left_own, left_sib, right_own, right_sib, out_ref):
        for at in range(0, left_dim, block):
            vals = lax.dot_general(left_own[:, at:at + block], right_own[ALL], ROW_DIMS, preferred_element_type=jnp.float32)
            out_ref[at:at + block, :] = vals + lax.dot_general(left_sib[:, at:at + block], right_sib[ALL], ROW_DIMS, preferred_element_type=jnp.float32)

    whole = pl.BlockSpec((tok_count, left_dim), lambda step: (0, 0))
    part = pl.BlockSpec((tok_count, tile), lambda step: (0, step))
    return pl.pallas_call(
        kernel,
        grid=(n_cols // tile,),
        in_specs=[whole, whole, part, part],
        out_specs=pl.BlockSpec((left_dim, tile), lambda step: (0, step)),
        out_shape=jax.ShapeDtypeStruct((left_dim, n_cols), jnp.float32),
        compiler_params=pltpu.CompilerParams(vmem_limit_bytes=MUCH_VMEM),
        cost_estimate=cost_of(4 * tok_count * left_dim * n_cols),
        name='grad_rows_of',
    )(*left, *right)


def fold_rows(slot_of, d_normed, slot_dy, slot_rows, gain_f32, n_dev):
    n_slots, width = slot_rows.shape
    tok_count = slot_of.shape[ROW]
    sizes = [BASE_CAP] * n_dev + [HEAVY_CAP - RELAY_ROWS, RELAY_ROWS]

    def kernel(at_ref, dn_ref, dy_ref, rows_ref, gain_ref, *out_refs):
        start = 0
        for out_ref, size in zip(out_refs, sizes):
            place = slice(start, start + size)
            slot = start + row_iota((size, tok_count))
            chooser = (slot == at_ref[ALL]).astype(jnp.float32).astype(jnp.bfloat16)
            d_norm = jnp.dot(chooser, dn_ref[ALL], preferred_element_type=jnp.float32)
            out_ref[ALL] = dy_ref[place] + norm_back(rows_ref[place].astype(jnp.float32), d_norm, gain_ref[ALL])
            start += size

    return pl.pallas_call(
        kernel,
        out_shape=tuple(jax.ShapeDtypeStruct((size, width), jnp.float32) for size in sizes),
        in_specs=[pl.BlockSpec(memory_space=pltpu.VMEM)] * 5,
        out_specs=tuple(pl.BlockSpec(memory_space=pltpu.VMEM) for _ in sizes),
        compiler_params=pltpu.CompilerParams(vmem_limit_bytes=MOST_VMEM),
        cost_estimate=cost_of(2 * tok_count * n_slots * width),
        name='fold_rows',
    )(slot_of.reshape(1, tok_count), d_normed, slot_dy, slot_rows, gain_f32.reshape(1, width))


def hop_send(vals, hop, n_dev):
    return lax.ppermute(vals, 'fsdp', [(dev, dev ^ hop) for dev in range(n_dev)])


def side_scatter(vals, n_dev):
    groups = [list(range(side, n_dev, 2)) for side in range(2)]
    return lax.psum_scatter(vals, 'fsdp', scatter_dimension=0, tiled=True, axis_index_groups=groups)


def solution(mesh):
    tok_spec = P(('dp', 'fsdp'), None)
    seq_spec = P(('dp', 'fsdp'), None, None)
    part_vec = P(('dp', 'fsdp'))
    vec_spec = P('fsdp')
    mat_spec = P('fsdp', None)

    def device_step(tok_ids, grad_out, emb_table, norm_gain, w_query, w_kv_down, kv_gain, w_kv_up, w_out):
        seq_count, seq_len = tok_ids.shape
        vocab_dev, d_model = emb_table.shape
        tok_count = seq_count * seq_len
        kv_rank = w_kv_down.shape[COL] - ROPE_DIM
        n_dev = mesh.shape['fsdp']
        my_dev = lax.axis_index('fsdp')
        side = lax.rem(my_dev, PAIR)
        n_slots = n_dev * BASE_CAP + HEAVY_CAP
        flat_ids = tok_ids.reshape(tok_count)
        grad_rows = grad_out.reshape(tok_count, d_model)

        owner, owner_rank, is_first, counts = plan_ids(flat_ids, vocab_dev, n_dev)

        def token_slots(turn):
            return slots_of(owner, owner_rank, my_dev, n_dev, turn)

        note = [slot_list(flat_ids, token_slots(0), is_first, n_slots), flat_ids, counts, norm_gain, kv_gain]
        note = jnp.concatenate([piece.astype(jnp.float32) for piece in note])
        note = jnp.pad(note, (0, -note.shape[ROW] % 128))
        notes = lax.all_gather(note, 'fsdp')
        ends = [0]
        for size in (n_slots, tok_count, n_dev, norm_gain.shape[ROW], kv_gain.shape[ROW]):
            ends.append(ends[-1] + size)
        all_slots, all_ids, all_counts, all_gains, all_kv_gains = (notes[:, low:high] for low, high in zip(ends[:-1], ends[1:]))
        all_slots, all_ids, all_counts = (piece.astype(jnp.int32) for piece in (all_slots, all_ids, all_counts))
        gain_f32, kv_gain_f32 = all_gains.reshape(-1), all_kv_gains.reshape(-1)
        caps = owner_cap(jnp.arange(n_dev))
        turns = jnp.max((all_counts + caps - 1) // caps)

        w_out_full = lax.all_gather(w_out, 'fsdp', tiled=True)
        query_shard, down_shard = after(tuple(arrange_weights(w_query, w_kv_down)), notes)
        w_query_full = lax.all_gather(query_shard, 'fsdp', tiled=True)
        w_down_full = lax.all_gather(down_shard, 'fsdp', tiled=True)

        def turn_lists(turn):
            def one_dev(ids, dev, turn):
                its_owner, its_rank, its_first, _ = plan_ids(ids, vocab_dev, n_dev)
                return slot_list(ids, slots_of(its_owner, its_rank, dev, n_dev, turn), its_first, n_slots)

            ids, turn = lax.optimization_barrier((all_ids, jnp.asarray(turn, jnp.int32)))
            return wanted_lists(jax.vmap(one_dev, (0, 0, None))(ids, jnp.arange(n_dev), turn), my_dev, n_dev)

        def spread_of(turn):
            return (token_slots(turn)[:, NEW] == jnp.arange(n_slots)[NEW, :]).astype(jnp.bfloat16)

        def fetch_rows(lists):
            return swap_rows(pick_rows(emb_table, lists, my_dev), n_dev)

        def expand(turn, slot_rows):
            return jnp.dot(spread_of(turn), slot_rows, preferred_element_type=jnp.float32).astype(jnp.bfloat16)

        def expand_more(step, have):
            rows = lax.fori_loop(1, turns, lambda turn, have: have + expand(turn, fetch_rows(turn_lists(turn))), expand(0, slot_rows))
            normed = rms_scale(rows, gain_f32)
            return (rows, normed) + side_blocks(normed, side, n_dev)

        lists = wanted_lists(all_slots, my_dev, n_dev)
        first_plan = table_plan(lists, my_dev, vocab_dev)
        work = (token_slots(0).reshape(1, tok_count), grad_rows, w_out_full)
        slot_rows, slot_dy, d_mix = swap_rows(pick_rows(emb_table, lists, my_dev), n_dev, work)
        many = (turns > 1).astype(jnp.int32)
        first_rows = tuple(expand_rows(token_slots(0), slot_rows, gain_f32, side, n_dev))
        tok_rows, normed, x_own, x_give = lax.fori_loop(0, many, expand_more, first_rows)

        w_up_full = lax.all_gather(after(w_kv_up, slot_rows), 'fsdp', tiled=True)
        down = jnp.dot(normed, w_down_full, preferred_element_type=jnp.float32).astype(jnp.bfloat16)
        latent, latent_pull = jax.vjp(rms_scale, down[:, :kv_rank], kv_gain_f32)
        kv_all = jnp.dot(latent, w_up_full, preferred_element_type=jnp.float32).astype(jnp.bfloat16)
        q_all = jnp.dot(normed, w_query_full, preferred_element_type=jnp.float32).astype(jnp.bfloat16)
        x_both = (x_own, hop_send(x_give, 1, n_dev))
        dy_both = (grad_rows, hop_send(grad_rows, 1, n_dev))
        latent_own, latent_give = side_blocks(latent, side, n_dev)
        latent_both = (latent_own, hop_send(latent_give, 1, n_dev))
        mix, mix_own, mix_give, d_query, d_up, d_pe = attend_pairs(q_all, kv_all, down[:, kv_rank:], d_mix, seq_count, side)

        dq_both = (d_query, hop_send(d_query, 1, n_dev))
        mix_both = (mix_own, hop_send(mix_give, 1, n_dev))
        dup_both = (d_up, hop_send(d_up, 1, n_dev))
        d_latent = lax.dot_general(d_up, w_up_full, COL_DIMS, preferred_element_type=jnp.float32).astype(jnp.bfloat16)
        d_w_query = grad_rows_of((after(x_both[0], d_latent), x_both[1]), dq_both)
        g_query = side_scatter(d_w_query, n_dev)
        d_ckv, d_kv_gain = latent_pull(after(d_latent, d_w_query))
        d_down = jnp.concatenate([d_ckv, d_pe], axis=COL)
        d_normed = lax.dot_general(after(d_query, d_w_query), w_query_full, COL_DIMS, preferred_element_type=jnp.float32)
        d_normed = d_normed + lax.dot_general(d_down, w_down_full, COL_DIMS, preferred_element_type=jnp.float32)
        d_normed = d_normed.astype(jnp.bfloat16)
        parts = fold_rows(token_slots(0), d_normed, slot_dy, slot_rows, gain_f32, n_dev)
        pieces = permute_rows(parts, n_dev)

        d_w_out = grad_rows_of((after(mix_both[0], *parts), mix_both[1]), dy_both)
        toks_f32 = after(tok_rows, d_w_out).astype(jnp.float32)
        gains = jnp.concatenate([gain_back(toks_f32, d_normed.astype(jnp.float32)), d_kv_gain])
        gains = gains + hop_send(gains, 1, n_dev)
        down_both = (after(d_down, d_w_out), hop_send(d_down, 1, n_dev))
        d_w_down = grad_rows_of(x_both, down_both, LANES)
        gain_col = lax.dynamic_index_in_dim(gains[:d_model].reshape(-1, 2, d_model // n_dev), side, 1, False)
        kv_gain_col = lax.dynamic_index_in_dim(gains[d_model:].reshape(-1, 2, kv_rank // n_dev), side, 1, False)
        kv_gain_col = jnp.pad(kv_gain_col, ((0, 0), (0, (d_model - kv_rank) // n_dev)))
        col_at = jnp.arange(d_w_down.shape[COL])[NEW, :]
        gain_at, kv_gain_at = kv_rank + HALF_ROPE, kv_rank + ROPE_DIM + HALF_ROPE
        d_w_down = jnp.where(col_at == gain_at, gain_col.reshape(-1, 1), jnp.where(col_at == kv_gain_at, kv_gain_col.reshape(-1, 1), d_w_down))
        d_w_out_down = jnp.concatenate([d_w_out, d_w_down], axis=COL)
        d_w_up = grad_rows_of((after(latent_both[0], d_w_out_down), latent_both[1]), dup_both)
        g_up = side_scatter(d_w_up, n_dev)
        block_out = (toks_f32 + jnp.dot(after(mix, d_w_up), w_out_full, preferred_element_type=jnp.float32)).astype(jnp.bfloat16)
        g_out_down = side_scatter(after(d_w_out_down, pieces, d_w_up, block_out), n_dev)
        g_out, g_down = g_out_down[:, :d_model], g_out_down[:, d_model:]

        def many_turns(step, table):
            d_rows = grad_rows.astype(jnp.float32) + norm_back(tok_rows.astype(jnp.float32), d_normed.astype(jnp.float32), gain_f32)

            def add_turn(turn, table):
                slot_grads = lax.dot_general(spread_of(turn).astype(jnp.float32), d_rows, ROW_DIMS, precision=lax.Precision.HIGHEST, preferred_element_type=jnp.float32)
                return write_table(return_rows(slot_grads, n_dev), table_plan(turn_lists(turn), my_dev, vocab_dev), my_dev, vocab_dev, jnp.float32, table)

            return lax.fori_loop(0, turns, add_turn, jnp.zeros((vocab_dev, d_model), jnp.float32)).astype(jnp.bfloat16)

        g_query = head_columns(g_query)
        grad_table = lax.fori_loop(0, many, many_turns, write_table(pieces, first_plan, my_dev, vocab_dev, jnp.bfloat16))
        g_pe = [g_down[:, kv_rank:kv_rank + HALF_ROPE], g_down[:, kv_rank + ROPE_DIM:kv_rank + ROPE_DIM + HALF_ROPE]]
        grads = (g_down[:, gain_at], g_query, jnp.concatenate([g_down[:, :kv_rank]] + g_pe, axis=COL), g_down[:kv_gain.shape[ROW], kv_gain_at], g_up, g_out)
        return (block_out.reshape(seq_count, seq_len, d_model), grad_table) + grads

    return jax.shard_map(device_step, mesh=mesh, in_specs=(tok_spec, seq_spec, mat_spec, vec_spec, mat_spec, mat_spec, vec_spec, mat_spec, mat_spec), out_specs=(seq_spec, tok_spec, part_vec, tok_spec, tok_spec, part_vec, tok_spec, tok_spec), check_vma=False)
```

```python
import math
import jax
import jax.numpy as jnp
from jax import lax
from jax.experimental import pallas as pl
from jax.experimental.pallas import tpu as pltpu
from jax.sharding import PartitionSpec as P

ALL, NEW = ..., None
ROW, COL, LAST = 0, 1, -1
TILE_ROWS, LANES, PAIR = 8, 128, 2
SMALL_FLOPS, LARGE_FLOPS, SOME_BYTES = 4 * 10**9, 2 * 10**10, 10**8
MUCH_VMEM, MOST_VMEM = 48 * 2**20, 60 * 2**20
NOPE_DIM = 128
ROPE_DIM = 64
VALUE_DIM = 128
ROPE_THETA = 50000.0
RMS_EPS = 1e-6
ATTN_SCALE = (NOPE_DIM + ROPE_DIM) ** -0.5 * (0.1 * math.log(32.0) + 1.0) ** 2
LOG2_E = math.log2(math.e)
ROW_DIMS = (((0,), (0,)), ((), ()))
COL_DIMS = (((1,), (1,)), ((), ()))
PAIR_DIM = 2 * (NOPE_DIM + ROPE_DIM)
HALF_ROPE = ROPE_DIM // 2
Q_ROWS = 256


def cost_of(flops):
    return pl.CostEstimate(flops=flops, bytes_accessed=SOME_BYTES, transcendentals=0)


def row_iota(shape):
    return lax.broadcasted_iota(jnp.int32, shape, ROW)


def col_iota(shape):
    return lax.broadcasted_iota(jnp.int32, shape, COL)


def rms_scale(in_vals, gain_vec):
    vals_f32 = in_vals.astype(jnp.float32)
    inv_rms = lax.rsqrt(jnp.mean(vals_f32 * vals_f32, axis=LAST, keepdims=True) + RMS_EPS)
    return (vals_f32 * inv_rms * gain_vec).astype(jnp.bfloat16)


def norm_back(rows_f32, d_normed, gain_vec):
    inv_rms = lax.rsqrt(jnp.mean(rows_f32 * rows_f32, axis=LAST, keepdims=True) + RMS_EPS)
    scaled = d_normed * gain_vec
    along = jnp.mean(scaled * rows_f32, axis=LAST, keepdims=True) * (inv_rms * inv_rms * inv_rms)
    return scaled * inv_rms - rows_f32 * along


def gain_back(rows_f32, d_normed):
    inv_rms = lax.rsqrt(jnp.mean(rows_f32 * rows_f32, axis=LAST, keepdims=True) + RMS_EPS)
    return jnp.sum(d_normed * (rows_f32 * inv_rms), axis=ROW)


def pair_source(width):
    at = jnp.arange(width)
    turned = at - 2 * NOPE_DIM
    part, head, i = turned // (2 * HALF_ROPE), lax.rem(turned // HALF_ROPE, PAIR), lax.rem(turned, HALF_ROPE)
    plain = (NOPE_DIM + ROPE_DIM) * (at // NOPE_DIM) + lax.rem(at, NOPE_DIM)
    return jnp.where(at < 2 * NOPE_DIM, plain, (NOPE_DIM + ROPE_DIM) * head + NOPE_DIM + HALF_ROPE * part + i)


def arrange_weights(w_query, w_down):
    rows, query_dim = w_query.shape
    kv_rank = w_down.shape[COL] - ROPE_DIM
    down_dim = kv_rank + 2 * ROPE_DIM
    pair_pick = (jnp.arange(PAIR_DIM)[:, NEW] == pair_source(PAIR_DIM)[NEW, :]).astype(w_query.dtype)
    twice = HALF_ROPE * (jnp.arange(2 * ROPE_DIM) // (2 * HALF_ROPE)) + lax.rem(jnp.arange(2 * ROPE_DIM), HALF_ROPE)
    twice_pick = (jnp.arange(ROPE_DIM)[:, NEW] == twice[NEW, :]).astype(w_query.dtype)

    def kernel(query_ref, down_ref, pair_ref, twice_ref, out_ref, low_ref):
        for at in range(0, query_dim, PAIR_DIM):
            out_ref[:, at:at + PAIR_DIM] = jnp.dot(query_ref[:, at:at + PAIR_DIM], pair_ref[ALL], preferred_element_type=jnp.float32).astype(out_ref.dtype)
        low_ref[:, :kv_rank] = down_ref[:, :kv_rank]
        low_ref[:, kv_rank:] = jnp.dot(down_ref[:, kv_rank:], twice_ref[ALL], preferred_element_type=jnp.float32).astype(low_ref.dtype)

    return pl.pallas_call(
        kernel,
        out_shape=(jax.ShapeDtypeStruct((rows, query_dim), w_query.dtype), jax.ShapeDtypeStruct((rows, down_dim), w_query.dtype)),
        in_specs=[pl.BlockSpec(memory_space=pltpu.VMEM)] * 4,
        out_specs=(pl.BlockSpec(memory_space=pltpu.VMEM),) * 2,
        cost_estimate=cost_of(SMALL_FLOPS),
        name='arrange_weights',
    )(w_query, w_down, pair_pick, twice_pick)


def heads_pick():
    return (jnp.arange(PAIR_DIM)[NEW, :] == pair_source(PAIR_DIM)[:, NEW]).astype(jnp.bfloat16)


def split_three(vals):
    high = vals.astype(jnp.bfloat16)
    left = vals - high.astype(jnp.float32)
    mid = left.astype(jnp.bfloat16)
    return high, mid, (left - mid.astype(jnp.float32)).astype(jnp.bfloat16)


def rope_tables(seq_len):
    positions = jnp.arange(seq_len, dtype=jnp.float32)
    inv_freq = ROPE_THETA ** (-2.0 * jnp.arange(HALF_ROPE, dtype=jnp.float32) / ROPE_DIM)
    rot_angle = positions[:, NEW] * inv_freq[NEW, :]
    cos_tab, sin_tab = jnp.cos(rot_angle), jnp.sin(rot_angle)
    return jnp.concatenate([cos_tab] * 4, axis=COL), jnp.concatenate([-sin_tab, -sin_tab, sin_tab, sin_tab], axis=COL)


def attend_pairs(q_all, kv_all, pe_all, d_mix, seq_count, side):
    tok_count = q_all.shape[ROW]
    seq_len = tok_count // seq_count
    n_pairs = q_all.shape[COL] // PAIR_DIM
    kv_dim = NOPE_DIM + VALUE_DIM
    cos_tab, sin_tab = rope_tables(seq_len)

    def kernel(side_s, q_ref, kv_ref, pe_ref, do_ref, cos_ref, sin_ref, mix_ref, own_ref, give_ref, dq_ref, dkv_ref, dpe_ref, key_acc):
        pair = pl.program_id(1)
        cos_vals, sin_vals = cos_ref[ALL], sin_ref[ALL]
        lane = col_iota((seq_len, 2 * ROPE_DIM))

        def turn(vals):
            return vals * cos_vals + pltpu.roll(vals, ROPE_DIM, 1) * sin_vals

        def turn_back(vals):
            return vals * cos_vals - pltpu.roll(vals, ROPE_DIM, 1) * sin_vals

        k_rot = turn(pe_ref[ALL].astype(jnp.float32)).astype(jnp.bfloat16)
        q_rot = turn(q_ref[:, 2 * NOPE_DIM:].astype(jnp.float32)).astype(jnp.bfloat16)
        n_blocks = seq_len // Q_ROWS
        d_q_rot = [None] * n_blocks
        d_k_rot = jnp.zeros((seq_len, 2 * ROPE_DIM), jnp.float32)
        in_head = [lax.rem(lane // HALF_ROPE, PAIR) == head for head in range(2)]
        keys = [jnp.concatenate([kv_ref[:, kv_dim * head:kv_dim * head + NOPE_DIM], jnp.where(in_head[head], k_rot, jnp.zeros_like(k_rot))], axis=COL) for head in range(2)]
        values = [kv_ref[:, kv_dim * head + NOPE_DIM:kv_dim * (head + 1)] for head in range(2)]
        queries = [jnp.concatenate([q_ref[:, NOPE_DIM * head:NOPE_DIM * (head + 1)], q_rot], axis=COL) for head in range(2)]
        d_out = [do_ref[:, VALUE_DIM * head:VALUE_DIM * (head + 1)] for head in range(2)]
        d_keys, d_values = {}, {}
        chains = [(head, block) for head in range(2) for block in range(n_blocks)]

        def first_dots(chain):
            head, block = chain
            rows, upto = slice(block * Q_ROWS, (block + 1) * Q_ROWS), (block + 1) * Q_ROWS
            scores = lax.dot_general(queries[head][rows], keys[head][:upto], COL_DIMS, preferred_element_type=jnp.float32)
            return scores, lax.dot_general(d_out[head][rows], values[head][:upto], COL_DIMS, preferred_element_type=jnp.float32)

        def softmax(chain, scores):
            _, block = chain
            row_at = block * Q_ROWS + row_iota(scores.shape)
            col_at = col_iota(scores.shape)
            scores = jnp.where(row_at >= col_at, scores, -1e30)
            powers = jnp.exp2((scores - jnp.max(scores, axis=LAST, keepdims=True)) * (ATTN_SCALE * LOG2_E))
            return powers * (1.0 / jnp.sum(powers, axis=LAST, keepdims=True))

        def last_dots(chain, probs, d_probs):
            head, block = chain
            rows, upto = slice(block * Q_ROWS, (block + 1) * Q_ROWS), (block + 1) * Q_ROWS
            probs_low = probs.astype(jnp.bfloat16)
            mixed = jnp.dot(probs_low, values[head][:upto], preferred_element_type=jnp.float32)
            mix_ref[rows, VALUE_DIM * head:VALUE_DIM * (head + 1)] = mixed.astype(jnp.bfloat16)
            leaning = jnp.sum(mixed * d_out[head][rows].astype(jnp.float32), axis=LAST, keepdims=True)
            d_scores = (probs * (d_probs - leaning)).astype(jnp.bfloat16)
            d_queries = jnp.dot(d_scores, keys[head][:upto], preferred_element_type=jnp.float32) * ATTN_SCALE
            dq_ref[rows, NOPE_DIM * head:NOPE_DIM * (head + 1)] = d_queries[:, :NOPE_DIM].astype(jnp.bfloat16)
            d_q_rot[block] = d_queries[:, NOPE_DIM:] if d_q_rot[block] is None else d_q_rot[block] + d_queries[:, NOPE_DIM:]
            key_part = lax.dot_general(d_scores, queries[head][rows], ROW_DIMS, preferred_element_type=jnp.float32)
            value_part = lax.dot_general(probs_low, d_out[head][rows], ROW_DIMS, preferred_element_type=jnp.float32)
            for below in range(block + 1):
                cut = slice(below * Q_ROWS, (below + 1) * Q_ROWS)
                for have, part in ((d_keys, key_part), (d_values, value_part)):
                    have[head, below] = have[head, below] + part[cut] if (head, below) in have else part[cut]

        ready = first_dots(chains[0])
        held = None
        for at, chain in enumerate(chains):
            scores, d_probs = ready
            if at + 1 < len(chains):
                ready = first_dots(chains[at + 1])
            if held is not None:
                last_dots(*held)
            held = (chain, softmax(chain, scores), d_probs)
        last_dots(*held)
        for head in range(2):
            all_keys = jnp.concatenate([d_keys[head, below] for below in range(n_blocks)], axis=ROW) * ATTN_SCALE
            dkv_ref[:, kv_dim * head:kv_dim * head + NOPE_DIM] = all_keys[:, :NOPE_DIM].astype(jnp.bfloat16)
            dkv_ref[:, kv_dim * head + NOPE_DIM:kv_dim * (head + 1)] = jnp.concatenate([d_values[head, below] for below in range(n_blocks)], axis=ROW).astype(jnp.bfloat16)
            d_k_rot = d_k_rot + jnp.where(in_head[head], all_keys[:, NOPE_DIM:], 0.0)
        dq_ref[:, 2 * NOPE_DIM:] = turn_back(jnp.concatenate(d_q_rot, axis=ROW)).astype(jnp.bfloat16)

        is_own = lax.rem(pair, PAIR) == side_s[0]

        @pl.when(is_own)
        def _():
            own_ref[ALL] = mix_ref[ALL]

        @pl.when(jnp.logical_not(is_own))
        def _():
            give_ref[ALL] = mix_ref[ALL]

        @pl.when(pair == 0)
        def _():
            key_acc[ALL] = d_k_rot

        @pl.when(pair > 0)
        def _():
            key_acc[ALL] += d_k_rot

        @pl.when(pair == n_pairs - 1)
        def _():
            both = key_acc[ALL]
            both = both + pltpu.roll(both, 2 * ROPE_DIM - HALF_ROPE, 1)
            both = jnp.where(lax.rem(lane // HALF_ROPE, PAIR) == 0, turn_back(both), 0.0)
            dpe_ref[ALL] = both.astype(jnp.bfloat16)

    def pair_block(width):
        return pl.BlockSpec((seq_len, width), lambda seq, pair, side: (seq, pair))

    half_block = pl.BlockSpec((seq_len, 2 * VALUE_DIM), lambda seq, pair, side: (seq, pair // 2))
    seq_block = pl.BlockSpec((seq_len, 2 * ROPE_DIM), lambda seq, pair, side: (seq, 0))
    tab_block = pl.BlockSpec((seq_len, 2 * ROPE_DIM), lambda seq, pair, side: (0, 0))
    shape = lambda width: jax.ShapeDtypeStruct((tok_count, width), jnp.bfloat16)
    return pl.pallas_call(
        kernel,
        grid_spec=pltpu.PrefetchScalarGridSpec(
            num_scalar_prefetch=1,
            grid=(seq_count, n_pairs),
            in_specs=[pair_block(PAIR_DIM), pair_block(2 * kv_dim), seq_block, pair_block(2 * VALUE_DIM), tab_block, tab_block],
            out_specs=(pair_block(2 * VALUE_DIM), half_block, half_block, pair_block(PAIR_DIM), pair_block(2 * kv_dim), seq_block),
            scratch_shapes=[pltpu.VMEM((seq_len, 2 * ROPE_DIM), jnp.float32)],
        ),
        out_shape=(shape(n_pairs * 2 * VALUE_DIM), shape(n_pairs * VALUE_DIM), shape(n_pairs * VALUE_DIM), shape(n_pairs * PAIR_DIM), shape(n_pairs * 2 * kv_dim), shape(2 * ROPE_DIM)),
        compiler_params=pltpu.CompilerParams(vmem_limit_bytes=MUCH_VMEM),
        cost_estimate=cost_of(LARGE_FLOPS),
        name='attend_pairs',
    )(side.reshape(1), q_all, kv_all, pe_all, d_mix, cos_tab, sin_tab)


BASE_CAP = 144
HEAVY_CAP = 480
RELAY_ROWS = 240
RELAY_PARTS = 3
DEST_ROWS = BASE_CAP + HEAVY_CAP
GROUP_ROWS = 48
FETCH_SLOTS = 6
TABLE_SLOTS = 4
SLOT_TILE = 136
MIX_TILE = 256
OUT_ROWS = 128
STEP_ROWS = 128
MESH_ID = pl.DeviceIdType.MESH


def shifted_sum(counts):
    size = counts.shape[LAST]
    lower = jnp.arange(size)[:, NEW] < jnp.arange(size)[NEW, :]
    return jnp.sum(jnp.where(lower, counts[ALL, :, None], 0), axis=-2)


def owner_cap(owner):
    return BASE_CAP + jnp.where(owner == 0, HEAVY_CAP, 0)


def plan_ids(flat_ids, vocab_dev, n_dev):
    order = jnp.arange(flat_ids.shape[ROW])
    same_before = (flat_ids[:, NEW] == flat_ids[NEW, :]) & (order[:, NEW] < order[NEW, :])
    is_first = jnp.logical_not(jnp.any(same_before, axis=ROW))
    lower = (flat_ids[:, NEW] < flat_ids[NEW, :]) & is_first[:, NEW]
    unique_rank = jnp.sum(lower.astype(jnp.int32), axis=ROW)
    owner = flat_ids // vocab_dev
    owned = owner[:, NEW] == jnp.arange(n_dev)[NEW, :]
    counts = jnp.sum((owned & is_first[:, NEW]).astype(jnp.int32), axis=ROW)
    owner_rank = unique_rank - jnp.sum(jnp.where(owned, shifted_sum(counts)[NEW, :], 0), axis=COL)
    return owner, owner_rank, is_first, counts


def slots_of(owner, owner_rank, dev, n_dev, turn):
    cap = owner_cap(owner)
    within = owner_rank - turn * cap
    slot = jnp.where(within < BASE_CAP, BASE_CAP * (owner ^ dev) + within, BASE_CAP * (n_dev - 1) + within)
    return jnp.where((within >= 0) & (within < cap), slot, -1)


def slot_list(flat_ids, slot_of, is_first, n_slots):
    hits = (slot_of[:, NEW] == jnp.arange(n_slots)[NEW, :]) & is_first[:, NEW]
    return jnp.sum(jnp.where(hits, flat_ids[:, NEW] + 1, 0), axis=ROW) - 1


def wanted_lists(all_slots, my_dev, n_dev):
    hop = jnp.arange(n_dev)[:, NEW] ^ my_dev
    base = all_slots[:, :n_dev * BASE_CAP].reshape(n_dev, n_dev, BASE_CAP)
    base = jnp.sum(jnp.where((hop == jnp.arange(n_dev)[NEW, :])[:, :, NEW], base, 0), axis=COL)
    heavy = jnp.where(my_dev == 0, all_slots[:, n_dev * BASE_CAP:], -1)
    by_dest = jnp.concatenate([base, heavy], axis=COL)
    return jnp.sum(jnp.where((hop == jnp.arange(n_dev)[NEW, :])[:, :, NEW], by_dest[:, NEW, :], 0), axis=ROW)


def pick_rows(table, lists, my_dev):
    vocab_dev, width = table.shape
    n_dev = lists.shape[ROW]
    flat = lists.reshape(-1)
    at = jnp.arange(n_dev * DEST_ROWS)
    local = jnp.where(flat < 0, lax.rem(TILE_ROWS * at, vocab_dev), jnp.clip(flat - my_dev * vocab_dev, 0, vocab_dev - 1))
    tiles = TILE_ROWS * (local // TILE_ROWS)
    tags = lax.rem(local, TILE_ROWS) + TILE_ROWS * lax.rem(at, GROUP_ROWS)
    tags = jnp.broadcast_to(tags[:, NEW], (n_dev * DEST_ROWS, LANES))
    all_groups = DEST_ROWS // GROUP_ROWS
    few_groups = -(-BASE_CAP // GROUP_ROWS)

    def kernel(tiles_s, dev_s, table_ref, tags_ref, out_ref, fetched, named, picked, fetch_sem, name_sem, out_sem):
        per_dest = jnp.where(dev_s[0] == 0, all_groups, few_groups)
        n_groups = n_dev * per_dest

        def row_at(group):
            dest = group // per_dest
            return pl.multiple_of(dest * DEST_ROWS + GROUP_ROWS * (group - dest * per_dest), GROUP_ROWS)

        def start_fetch(group):
            slot = lax.rem(group, FETCH_SLOTS)
            row = row_at(jnp.minimum(group, n_groups - 1))
            pltpu.make_async_copy(tags_ref.at[pl.ds(row, GROUP_ROWS)], named.at[slot], name_sem.at[slot]).start()
            for i in range(GROUP_ROWS):
                pltpu.make_async_copy(table_ref.at[pl.ds(pl.multiple_of(tiles_s[row + i], TILE_ROWS), TILE_ROWS)], fetched.at[slot, pl.ds(TILE_ROWS * i, TILE_ROWS)], fetch_sem.at[slot]).start()

        def wait_fetch(slot):
            pltpu.make_async_copy(named.at[slot], named.at[slot], name_sem.at[slot]).wait()
            pltpu.make_async_copy(fetched.at[slot], fetched.at[slot], fetch_sem.at[slot]).wait()

        def out_copy(group):
            slot = lax.rem(group, TABLE_SLOTS)
            return pltpu.make_async_copy(picked.at[slot], out_ref.at[pl.ds(row_at(group), GROUP_ROWS)], out_sem.at[slot])

        for ahead in range(FETCH_SLOTS - 1):
            start_fetch(jnp.int32(ahead))

        def body(group, carry):
            @pl.when(group >= TABLE_SLOTS)
            def _():
                out_copy(group - TABLE_SLOTS).wait()

            slot = lax.rem(group, FETCH_SLOTS)
            wait_fetch(slot)
            start_fetch(group + FETCH_SLOTS - 1)
            lane = col_iota((GROUP_ROWS, LANES))
            name = named[slot]
            chooser = jnp.concatenate([(name == lane + at).astype(jnp.float32) for at in range(0, TILE_ROWS * GROUP_ROWS, LANES)], axis=COL).astype(jnp.bfloat16)
            picked[lax.rem(group, TABLE_SLOTS)] = jnp.dot(chooser, fetched[slot], preferred_element_type=jnp.float32).astype(jnp.bfloat16)
            out_copy(group).start()
            return carry

        lax.fori_loop(0, n_groups, body, 0)
        for ahead in range(FETCH_SLOTS - 1):
            wait_fetch(lax.rem(n_groups + ahead, FETCH_SLOTS))
        for back in range(TABLE_SLOTS, 0, -1):
            out_copy(n_groups - back).wait()

    return pl.pallas_call(
        kernel,
        out_shape=jax.ShapeDtypeStruct((n_dev * DEST_ROWS, width), table.dtype),
        grid_spec=pltpu.PrefetchScalarGridSpec(
            num_scalar_prefetch=2,
            grid=(1,),
            in_specs=[pl.BlockSpec(memory_space=pl.ANY)] * 2,
            out_specs=pl.BlockSpec(memory_space=pl.ANY),
            scratch_shapes=[
                pltpu.VMEM((FETCH_SLOTS, TILE_ROWS * GROUP_ROWS, width), table.dtype),
                pltpu.VMEM((FETCH_SLOTS, GROUP_ROWS, LANES), jnp.int32),
                pltpu.VMEM((TABLE_SLOTS, GROUP_ROWS, width), table.dtype),
                pltpu.SemaphoreType.DMA((FETCH_SLOTS,)),
                pltpu.SemaphoreType.DMA((FETCH_SLOTS,)),
                pltpu.SemaphoreType.DMA((TABLE_SLOTS,)),
            ],
        ),
        cost_estimate=cost_of(SMALL_FLOPS),
        name='pick_rows',
    )(tiles, my_dev.reshape(1), table, tags)


def greet_all(my_dev, n_dev):
    barrier = pltpu.get_barrier_semaphore()
    for hop in range(1, n_dev):
        pl.semaphore_signal(barrier, inc=1, device_id={'fsdp': my_dev ^ hop}, device_id_type=MESH_ID)
    pl.semaphore_wait(barrier, n_dev - 1)


def remote(source, target, send_sem, recv_sem, dest):
    return pltpu.make_async_remote_copy(src_ref=source, dst_ref=target, send_sem=send_sem, recv_sem=recv_sem, device_id={'fsdp': dest}, device_id_type=MESH_ID)


def swap_rows(picked, n_dev, work=None):
    width = picked.shape[LAST]
    n_slots = n_dev * BASE_CAP + HEAVY_CAP
    n_tiles = n_slots // SLOT_TILE
    tok_count = 0 if work is None else work[1].shape[ROW]
    heavy_at = n_dev * BASE_CAP
    part_rows = RELAY_ROWS // RELAY_PARTS

    def kernel(*refs):
        if work is None:
            in_ref, out_ref, relay_ref, local, send_sem, recv_sem, relay_send, relay_recv, local_sem = refs
        else:
            in_ref, at_ref, dy_ref, w_out_ref, out_ref, relay_ref, sums_ref, mix_ref, local, send_sem, recv_sem, relay_send, relay_recv, local_sem, dy_vals, w_vals, sums, mixes, load_sem, store_sem = refs
        my_dev = lax.axis_index('fsdp')
        greet_all(my_dev, n_dev)

        def base_copy(hop):
            return remote(in_ref.at[pl.ds(hop * DEST_ROWS, BASE_CAP)], out_ref.at[pl.ds(hop * BASE_CAP, BASE_CAP)], send_sem.at[hop], recv_sem.at[hop], my_dev ^ hop)

        def heavy_copy(dest):
            rows = HEAVY_CAP - (RELAY_ROWS if dest >= 6 else 0)
            return remote(in_ref.at[pl.ds(dest * DEST_ROWS + BASE_CAP, rows)], out_ref.at[pl.ds(heavy_at, rows)], send_sem.at[7 + dest], recv_sem.at[8], jnp.int32(dest))

        def relay_in(dest, part):
            at = dest * DEST_ROWS + DEST_ROWS - RELAY_ROWS + part * part_rows
            return remote(in_ref.at[pl.ds(at, part_rows)], relay_ref.at[pl.ds(part * part_rows, part_rows)], relay_send.at[dest - 6, part], relay_recv.at[part], jnp.int32(dest - 2))

        def relay_out(dest, part):
            at = heavy_at + HEAVY_CAP - RELAY_ROWS + part * part_rows
            return remote(relay_ref.at[pl.ds(part * part_rows, part_rows)], out_ref.at[pl.ds(at, part_rows)], relay_send.at[0, part], relay_recv.at[part], jnp.int32(dest))

        @pl.when(my_dev == 0)
        def _():
            for part in range(RELAY_PARTS):
                for dest in (6, 7):
                    relay_in(dest, part).start()
            for dest in (6, 7, 2, 4, 3, 5, 1):
                heavy_copy(dest).start()

        for hop in (6, 7, 2, 4, 3, 5, 1):
            base_copy(hop).start()
        if work is not None:
            loads = (pltpu.make_async_copy(dy_ref, dy_vals, load_sem.at[0]), pltpu.make_async_copy(w_out_ref, w_vals, load_sem.at[1]))
            for load in loads:
                load.start()
        own = pltpu.make_async_copy(in_ref.at[pl.ds(0, DEST_ROWS)], local, local_sem.at[0])
        own.start()
        own.wait()
        back = pltpu.make_async_copy(local.at[pl.ds(0, BASE_CAP)], out_ref.at[pl.ds(0, BASE_CAP)], local_sem.at[1])
        back.start()

        @pl.when(my_dev == 0)
        def _():
            mine = pltpu.make_async_copy(local.at[pl.ds(BASE_CAP, HEAVY_CAP)], out_ref.at[pl.ds(heavy_at, HEAVY_CAP)], local_sem.at[2])
            mine.start()
            mine.wait()

        back.wait()
        if work is not None:
            def sums_copy(tile):
                return pltpu.make_async_copy(sums.at[lax.rem(tile, PAIR)], sums_ref.at[pl.ds(pl.multiple_of(tile * SLOT_TILE, TILE_ROWS), SLOT_TILE)], store_sem.at[lax.rem(tile, PAIR)])

            def mix_copy(tile):
                return pltpu.make_async_copy(mixes.at[lax.rem(tile, PAIR)], mix_ref.at[pl.ds(pl.multiple_of(tile * MIX_TILE, TILE_ROWS), MIX_TILE)], store_sem.at[2 + lax.rem(tile, PAIR)])

            def sum_tile(tile, carry):
                @pl.when(tile >= 2)
                def _():
                    sums_copy(tile - 2).wait()

                slot = tile * SLOT_TILE + row_iota((SLOT_TILE, tok_count))
                chooser = (slot == at_ref[ALL]).astype(jnp.float32).astype(jnp.bfloat16)
                sums[lax.rem(tile, PAIR)] = jnp.dot(chooser, dy_vals[ALL], preferred_element_type=jnp.float32)
                sums_copy(tile).start()
                return carry

            def mix_tile(tile, carry):
                @pl.when(tile >= 2)
                def _():
                    mix_copy(tile - 2).wait()

                rows = dy_vals[pl.ds(pl.multiple_of(tile * MIX_TILE, MIX_TILE), MIX_TILE)]
                mixes[lax.rem(tile, PAIR)] = lax.dot_general(rows, w_vals[ALL], COL_DIMS, preferred_element_type=jnp.float32).astype(jnp.bfloat16)
                mix_copy(tile).start()
                return carry

            loads[0].wait()
            lax.fori_loop(0, n_tiles, sum_tile, 0)
        for mid in (4, 5):
            @pl.when(my_dev == mid)
            def _(mid=mid):
                for part in range(RELAY_PARTS):
                    relay_in(mid + 2, part).wait_recv()
                    relay_out(mid + 2, part).start()
                for part in range(RELAY_PARTS):
                    relay_out(mid + 2, part).wait_send()
        if work is not None:
            loads[1].wait()
            lax.fori_loop(0, tok_count // MIX_TILE, mix_tile, 0)
            for back_at in (2, 1):
                sums_copy(jnp.int32(n_tiles - back_at)).wait()
                mix_copy(jnp.int32(tok_count // MIX_TILE - back_at)).wait()
        for hop in range(1, n_dev):
            base_copy(hop).wait()
        for dest in range(1, n_dev):
            @pl.when(my_dev == dest)
            def _(dest=dest):
                heavy_copy(dest).wait_recv()
                if dest >= 6:
                    for part in range(RELAY_PARTS):
                        relay_out(dest, part).wait_recv()

            @pl.when(my_dev == 0)
            def _(dest=dest):
                heavy_copy(dest).wait_send()
                if dest >= 6:
                    for part in range(RELAY_PARTS):
                        relay_in(dest, part).wait_send()

    any_spec = pl.BlockSpec(memory_space=pl.ANY)
    out_shape = [jax.ShapeDtypeStruct((n_slots, width), picked.dtype), jax.ShapeDtypeStruct((RELAY_ROWS, width), picked.dtype)]
    in_specs = [any_spec]
    scratch_shapes = [
        pltpu.VMEM((DEST_ROWS, width), picked.dtype),
        pltpu.SemaphoreType.DMA((15,)),
        pltpu.SemaphoreType.DMA((9,)),
        pltpu.SemaphoreType.DMA((2, RELAY_PARTS)),
        pltpu.SemaphoreType.DMA((RELAY_PARTS,)),
        pltpu.SemaphoreType.DMA((3,)),
    ]
    if work is not None:
        in_specs += [pl.BlockSpec(memory_space=pltpu.VMEM), any_spec, any_spec]
        out_shape += [jax.ShapeDtypeStruct((n_slots, width), jnp.float32), jax.ShapeDtypeStruct((tok_count, work[2].shape[ROW]), jnp.bfloat16)]
        scratch_shapes += [
            pltpu.VMEM(work[1].shape, work[1].dtype),
            pltpu.VMEM(work[2].shape, work[2].dtype),
            pltpu.VMEM((2, SLOT_TILE, width), jnp.float32),
            pltpu.VMEM((2, MIX_TILE, work[2].shape[ROW]), jnp.bfloat16),
            pltpu.SemaphoreType.DMA((2,)),
            pltpu.SemaphoreType.DMA((4,)),
        ]
    outs = pl.pallas_call(
        kernel,
        out_shape=tuple(out_shape),
        in_specs=in_specs,
        out_specs=(any_spec,) * len(out_shape),
        scratch_shapes=scratch_shapes,
        compiler_params=pltpu.CompilerParams(collective_id=1 if work is None else 3, has_side_effects=True, vmem_limit_bytes=MUCH_VMEM),
        cost_estimate=cost_of(LARGE_FLOPS),
        name='swap_rows',
    )(picked, *(work or ()))
    return outs[0] if work is None else (outs[0], outs[2], outs[3])


def table_parts(source):
    if source < 6:
        return ((0, BASE_CAP), (BASE_CAP, HEAVY_CAP))
    return ((0, BASE_CAP), (BASE_CAP, HEAVY_CAP - RELAY_ROWS), (DEST_ROWS - RELAY_ROWS, RELAY_ROWS))


def permute_rows(parts, n_dev):
    base, direct, relayed = parts[:n_dev], parts[n_dev], parts[n_dev + 1]
    heavy = jnp.concatenate([direct, relayed], axis=ROW)
    passed = lax.ppermute(relayed, 'fsdp', [(6, 2), (7, 3)])
    arrived = {0: [heavy]}
    for source in (6, 7):
        arrived[source] = [lax.ppermute(direct, 'fsdp', [(source, 0)])]
    for source in (2, 4, 3, 5, 1):
        arrived[source] = [lax.ppermute(heavy, 'fsdp', [(source, 0)])]
    for source in (6, 7):
        arrived[source].append(lax.ppermute(passed, 'fsdp', [(source - 4, 0)]))
    base = [base[0]] + [lax.ppermute(base[hop], 'fsdp', [(dev, dev ^ hop) for dev in range(n_dev)]) for hop in range(1, n_dev)]
    return [piece for source in range(n_dev) for piece in [base[source]] + arrived[source]]


def return_rows(slot_grads, n_dev):
    width = slot_grads.shape[LAST]
    heavy_at = n_dev * BASE_CAP

    def kernel(in_ref, out_ref, local, send_sem, recv_sem, local_sem):
        my_dev = lax.axis_index('fsdp')
        greet_all(my_dev, n_dev)

        def base_copy(hop):
            place = pl.ds(hop * BASE_CAP, BASE_CAP)
            return remote(in_ref.at[place], out_ref.at[place], send_sem.at[hop], recv_sem.at[hop], my_dev ^ hop)

        def heavy_copy(source):
            return remote(in_ref.at[pl.ds(heavy_at, HEAVY_CAP)], out_ref.at[pl.ds(heavy_at + source * HEAVY_CAP, HEAVY_CAP)], send_sem.at[8], recv_sem.at[7 + source], jnp.int32(0))

        for source in range(1, n_dev):
            @pl.when(my_dev == source)
            def _(source=source):
                heavy_copy(source).start()
        for hop in range(1, n_dev):
            base_copy(hop).start()

        def bounce(at, rows):
            for one in (pltpu.make_async_copy(in_ref.at[pl.ds(at, rows)], local.at[pl.ds(0, rows)], local_sem), pltpu.make_async_copy(local.at[pl.ds(0, rows)], out_ref.at[pl.ds(at, rows)], local_sem)):
                one.start()
                one.wait()

        bounce(0, BASE_CAP)

        @pl.when(my_dev == 0)
        def _():
            bounce(heavy_at, HEAVY_CAP)

        for hop in range(1, n_dev):
            base_copy(hop).wait()
        for source in range(1, n_dev):
            @pl.when(my_dev == source)
            def _(source=source):
                heavy_copy(source).wait_send()

            @pl.when(my_dev == 0)
            def _(source=source):
                heavy_copy(source).wait_recv()

    arrived = pl.pallas_call(
        kernel,
        out_shape=jax.ShapeDtypeStruct((n_dev * DEST_ROWS, width), slot_grads.dtype),
        in_specs=[pl.BlockSpec(memory_space=pl.ANY)],
        out_specs=pl.BlockSpec(memory_space=pl.ANY),
        scratch_shapes=[
            pltpu.VMEM((HEAVY_CAP, width), slot_grads.dtype),
            pltpu.SemaphoreType.DMA((9,)),
            pltpu.SemaphoreType.DMA((15,)),
            pltpu.SemaphoreType.DMA,
        ],
        compiler_params=pltpu.CompilerParams(collective_id=2, has_side_effects=True),
        cost_estimate=cost_of(SMALL_FLOPS),
        name='return_rows',
    )(slot_grads)
    pieces = []
    for source in range(n_dev):
        pieces.append(arrived[source * BASE_CAP:(source + 1) * BASE_CAP])
        heavy_part = arrived[heavy_at + source * HEAVY_CAP:heavy_at + (source + 1) * HEAVY_CAP]
        pieces += [heavy_part[start - BASE_CAP:start - BASE_CAP + rows] for start, rows in table_parts(source)[1:]]
    return pieces


def table_plan(lists, my_dev, vocab_dev):
    n_dev = lists.shape[ROW]
    n_out = vocab_dev // OUT_ROWS
    edges = my_dev * vocab_dev + OUT_ROWS * jnp.arange(n_out + 1)
    below = (lists[NEW, :, :] >= 0) & (lists[NEW, :, :] < edges[:, NEW, NEW])
    upto = jnp.sum(below.astype(jnp.int32), axis=LAST)
    low, high = upto[:-1], upto[1:]
    firsts = low // TILE_ROWS
    counts = jnp.where(high > low, (high + 7) // TILE_ROWS - firsts, 0)
    names = jnp.broadcast_to(lists.reshape(-1, 1), (n_dev * DEST_ROWS, LANES))
    return firsts.reshape(-1), counts.reshape(-1), names


def write_table(pieces, plan, my_dev, vocab_dev, out_dtype, so_far=None):
    firsts, counts, names = plan
    width = pieces[0].shape[LAST]
    n_out = vocab_dev // OUT_ROWS
    n_part = len(pieces)
    n_source = firsts.shape[ROW] // n_out
    tile_blocks = OUT_ROWS // TILE_ROWS
    cap_rows = TILE_ROWS * n_source * (tile_blocks + 1)
    cap_rows = -(-cap_rows // STEP_ROWS) * STEP_ROWS

    def kernel(firsts_s, counts_s, dev_s, *refs):
        part_refs, names_ref = refs[:n_part], refs[n_part]
        old_ref = refs[n_part + 1] if so_far is not None else None
        out_ref, staged, named, total, ready, filled_s, row_sem, out_sem, old_sem = refs[-9:]

        def start_fetch(block):
            slot = lax.rem(block, TABLE_SLOTS)
            where = jnp.int32(0)
            first_ref = 0
            for source in range(n_source):
                parts = table_parts(source)
                first = firsts_s[block * n_source + source]

                def one(i, at, parts=parts, source=source, first=first, first_ref=first_ref):
                    block_at = first + i
                    place = pl.ds(pl.multiple_of(TILE_ROWS * at, TILE_ROWS), TILE_ROWS)
                    named[slot, place] = names_ref[pl.ds(pl.multiple_of(source * DEST_ROWS + TILE_ROWS * block_at, TILE_ROWS), TILE_ROWS)]
                    for part, (start, rows) in enumerate(parts):
                        @pl.when((block_at >= start // TILE_ROWS) & (block_at < (start + rows) // TILE_ROWS))
                        def _(part=part, start=start):
                            pltpu.make_async_copy(part_refs[first_ref + part].at[pl.ds(pl.multiple_of(TILE_ROWS * block_at - start, TILE_ROWS), TILE_ROWS)], staged.at[slot, place], row_sem.at[slot]).start()
                    return at + 1

                where = lax.fori_loop(0, counts_s[block * n_source + source], one, where)
                first_ref += len(parts)
            filled_s[slot] = where

        def out_copy(block):
            slot = lax.rem(block, TABLE_SLOTS)
            return pltpu.make_async_copy(ready.at[slot], out_ref.at[pl.ds(pl.multiple_of(block * OUT_ROWS, OUT_ROWS), OUT_ROWS)], out_sem.at[slot])

        for ahead in range(TABLE_SLOTS - 1):
            start_fetch(jnp.int32(ahead))

        def body(out_block, carry):
            @pl.when(out_block + TABLE_SLOTS - 1 < n_out)
            def _():
                start_fetch(out_block + TABLE_SLOTS - 1)

            @pl.when(out_block >= TABLE_SLOTS)
            def _():
                out_copy(out_block - TABLE_SLOTS).wait()

            slot = lax.rem(out_block, TABLE_SLOTS)
            n_blocks = filled_s[slot]

            def wait_one(i, carry):
                pltpu.make_async_copy(staged.at[slot, pl.ds(0, TILE_ROWS)], staged.at[slot, pl.ds(0, TILE_ROWS)], row_sem.at[slot]).wait()
                return carry

            lax.fori_loop(0, n_blocks, wait_one, 0)
            low_row = dev_s[0] * vocab_dev + out_block * OUT_ROWS

            def summed(start, rows, store):
                place = pl.ds(start, rows)
                live = start + row_iota((rows, OUT_ROWS)) < TILE_ROWS * n_blocks
                lane = col_iota((rows, OUT_ROWS))
                chooser = ((named[slot, place] - low_row == lane) & live).astype(jnp.float32)
                chooser = jnp.concatenate([chooser] * 3, axis=ROW).T.astype(jnp.bfloat16)
                for col in range(0, width, 512):
                    part = jnp.where(live[:, :1], staged[slot, place, col:col + 512], 0.0)
                    stacked = jnp.concatenate(split_three(part), axis=ROW)
                    store(col, jnp.dot(chooser, stacked, preferred_element_type=jnp.float32))

            def store_out(col, vals):
                ready[slot, :, col:col + 512] = vals.astype(out_dtype)

            def store_more(col, vals):
                total[:, col:col + 512] += vals

            few = jnp.int32(-1) if so_far is not None else n_blocks

            @pl.when(few == 0)
            def _():
                ready[slot] = jnp.zeros((OUT_ROWS, width), out_dtype)

            @pl.when((few > 0) & (few <= STEP_ROWS // 16))
            def _():
                summed(0, STEP_ROWS // 2, store_out)

            @pl.when((few > STEP_ROWS // 16) & (few <= STEP_ROWS // TILE_ROWS))
            def _():
                summed(0, STEP_ROWS, store_out)

            @pl.when((few < 0) | (few > STEP_ROWS // TILE_ROWS))
            def _():
                if so_far is None:
                    total[ALL] = jnp.zeros_like(total)
                else:
                    old = pltpu.make_async_copy(old_ref.at[pl.ds(pl.multiple_of(out_block * OUT_ROWS, OUT_ROWS), OUT_ROWS)], total, old_sem)
                    old.start()
                    old.wait()

                def add_step(step, carry):
                    summed(pl.multiple_of(step * STEP_ROWS, STEP_ROWS), STEP_ROWS, store_more)
                    return carry

                lax.fori_loop(0, (TILE_ROWS * n_blocks + STEP_ROWS - 1) // STEP_ROWS, add_step, 0)
                ready[slot] = total[ALL].astype(out_dtype)

            out_copy(out_block).start()
            return carry

        lax.fori_loop(0, n_out, body, 0)
        for back in range(TABLE_SLOTS, 0, -1):
            out_copy(n_out - back).wait()

    extra = () if so_far is None else (so_far,)
    any_spec = pl.BlockSpec(memory_space=pl.ANY)
    return pl.pallas_call(
        kernel,
        out_shape=jax.ShapeDtypeStruct((vocab_dev, width), out_dtype),
        grid_spec=pltpu.PrefetchScalarGridSpec(
            num_scalar_prefetch=3,
            grid=(1,),
            in_specs=[any_spec] * n_part + [pl.BlockSpec(names.shape, lambda i, *_: (0, 0))] + [any_spec] * len(extra),
            out_specs=any_spec,
            scratch_shapes=[
                pltpu.VMEM((TABLE_SLOTS, cap_rows, width), jnp.float32),
                pltpu.VMEM((TABLE_SLOTS, cap_rows, LANES), jnp.int32),
                pltpu.VMEM((OUT_ROWS, width), jnp.float32),
                pltpu.VMEM((TABLE_SLOTS, OUT_ROWS, width), out_dtype),
                pltpu.SMEM((TABLE_SLOTS,), jnp.int32),
                pltpu.SemaphoreType.DMA((TABLE_SLOTS,)),
                pltpu.SemaphoreType.DMA((TABLE_SLOTS,)),
                pltpu.SemaphoreType.DMA,
            ],
        ),
        compiler_params=pltpu.CompilerParams(vmem_limit_bytes=MOST_VMEM),
        cost_estimate=cost_of(SMALL_FLOPS),
        name='write_table',
    )(firsts, counts, my_dev.reshape(1), *pieces, names, *extra)


GRAD_TILE = 512
NORM_ROWS = 256


def after(vals, *deps):
    return lax.optimization_barrier((vals,) + deps)[0]


def side_blocks(rows, side, n_dev):
    block = rows.shape[COL] // n_dev
    cuts = [rows[:, at * block:(at + 1) * block] for at in range(n_dev)]
    even, odd = jnp.concatenate(cuts[0::2], axis=COL), jnp.concatenate(cuts[1::2], axis=COL)
    return jnp.where(side == 0, even, odd), jnp.where(side == 0, odd, even)


def expand_rows(slot_of, slot_rows, gain_f32, side, n_dev):
    n_slots, width = slot_rows.shape
    tok_count = slot_of.shape[ROW]
    slot_cols = jnp.broadcast_to(slot_of[:, NEW], (tok_count, LANES))

    def kernel(side_s, at_ref, rows_ref, gain_ref, tok_ref, norm_ref, own_ref, give_ref):
        lane = col_iota((NORM_ROWS, n_slots))
        chooser = (at_ref[:, :1] == lane).astype(jnp.float32).astype(jnp.bfloat16)
        vals = jnp.dot(chooser, rows_ref[ALL], preferred_element_type=jnp.float32)
        tok_ref[ALL] = vals.astype(jnp.bfloat16)
        inv_rms = lax.rsqrt(jnp.mean(vals * vals, axis=LAST, keepdims=True) + RMS_EPS)
        normed = (vals * inv_rms * gain_ref[ALL]).astype(jnp.bfloat16)
        norm_ref[ALL] = normed
        own_ref[ALL], give_ref[ALL] = side_blocks(normed, side_s[0], n_dev)

    def row_block(cols):
        return pl.BlockSpec((NORM_ROWS, cols), lambda step, side: (step, 0))

    def whole(rows):
        return pl.BlockSpec((rows, width), lambda step, side: (0, 0))

    shape = lambda cols: jax.ShapeDtypeStruct((tok_count, cols), jnp.bfloat16)
    return pl.pallas_call(
        kernel,
        grid_spec=pltpu.PrefetchScalarGridSpec(
            num_scalar_prefetch=1,
            grid=(tok_count // NORM_ROWS,),
            in_specs=[row_block(128), whole(n_slots), whole(1)],
            out_specs=(row_block(width), row_block(width), row_block(width // 2), row_block(width // 2)),
        ),
        out_shape=(shape(width), shape(width), shape(width // 2), shape(width // 2)),
        compiler_params=pltpu.CompilerParams(vmem_limit_bytes=MUCH_VMEM),
        cost_estimate=cost_of(2 * tok_count * n_slots * width),
        name='expand_rows',
    )(side.reshape(1), slot_cols, slot_rows, gain_f32.reshape(1, width))


def grad_rows_of(left, right, tile=GRAD_TILE, pick=None):
    tok_count, left_dim = left[0].shape
    n_cols = right[0].shape[COL]
    block = 256

    def columns(right_ref, pick_refs):
        if not pick_refs:
            return right_ref[ALL]
        cuts = [right_ref[:, at:at + PAIR_DIM] for at in range(0, tile, PAIR_DIM)]
        return jnp.concatenate([jnp.dot(cut, pick_refs[0][ALL], preferred_element_type=jnp.float32).astype(jnp.bfloat16) for cut in cuts], axis=COL)

    def kernel(left_own, left_sib, right_own, right_sib, *rest):
        out_ref = rest[-1]
        own_cols, sib_cols = columns(right_own, rest[:-1]), columns(right_sib, rest[:-1])
        for at in range(0, left_dim, block):
            vals = lax.dot_general(left_own[:, at:at + block], own_cols, ROW_DIMS, preferred_element_type=jnp.float32)
            out_ref[at:at + block, :] = vals + lax.dot_general(left_sib[:, at:at + block], sib_cols, ROW_DIMS, preferred_element_type=jnp.float32)

    whole = pl.BlockSpec((tok_count, left_dim), lambda step: (0, 0))
    part = pl.BlockSpec((tok_count, tile), lambda step: (0, step))
    extras = () if pick is None else (pick,)
    return pl.pallas_call(
        kernel,
        grid=(n_cols // tile,),
        in_specs=[whole, whole, part, part] + [pl.BlockSpec(extra.shape, lambda step: (0, 0)) for extra in extras],
        out_specs=pl.BlockSpec((left_dim, tile), lambda step: (0, step)),
        out_shape=jax.ShapeDtypeStruct((left_dim, n_cols), jnp.float32),
        compiler_params=pltpu.CompilerParams(vmem_limit_bytes=MUCH_VMEM),
        cost_estimate=cost_of(4 * tok_count * left_dim * n_cols),
        name='grad_rows_of',
    )(*left, *right, *extras)


def fold_rows(slot_of, d_normed, slot_dy, slot_rows, gain_f32, n_dev):
    n_slots, width = slot_rows.shape
    tok_count = slot_of.shape[ROW]
    sizes = [BASE_CAP] * n_dev + [HEAVY_CAP - RELAY_ROWS, RELAY_ROWS]

    def kernel(at_ref, dn_ref, dy_ref, rows_ref, gain_ref, *out_refs):
        start = 0
        for out_ref, size in zip(out_refs, sizes):
            place = slice(start, start + size)
            slot = start + row_iota((size, tok_count))
            chooser = (slot == at_ref[ALL]).astype(jnp.float32).astype(jnp.bfloat16)
            d_norm = jnp.dot(chooser, dn_ref[ALL], preferred_element_type=jnp.float32)
            out_ref[ALL] = dy_ref[place] + norm_back(rows_ref[place].astype(jnp.float32), d_norm, gain_ref[ALL])
            start += size

    return pl.pallas_call(
        kernel,
        out_shape=tuple(jax.ShapeDtypeStruct((size, width), jnp.float32) for size in sizes),
        in_specs=[pl.BlockSpec(memory_space=pltpu.VMEM)] * 5,
        out_specs=tuple(pl.BlockSpec(memory_space=pltpu.VMEM) for _ in sizes),
        compiler_params=pltpu.CompilerParams(vmem_limit_bytes=MOST_VMEM),
        cost_estimate=cost_of(2 * tok_count * n_slots * width),
        name='fold_rows',
    )(slot_of.reshape(1, tok_count), d_normed, slot_dy, slot_rows, gain_f32.reshape(1, width))


def hop_send(vals, hop, n_dev):
    return lax.ppermute(vals, 'fsdp', [(dev, dev ^ hop) for dev in range(n_dev)])


def side_scatter(vals, n_dev):
    groups = [list(range(side, n_dev, 2)) for side in range(2)]
    return lax.psum_scatter(vals, 'fsdp', scatter_dimension=0, tiled=True, axis_index_groups=groups)


def solution(mesh):
    tok_spec = P(('dp', 'fsdp'), None)
    seq_spec = P(('dp', 'fsdp'), None, None)
    part_vec = P(('dp', 'fsdp'))
    vec_spec = P('fsdp')
    mat_spec = P('fsdp', None)

    def device_step(tok_ids, grad_out, emb_table, norm_gain, w_query, w_kv_down, kv_gain, w_kv_up, w_out):
        seq_count, seq_len = tok_ids.shape
        vocab_dev, d_model = emb_table.shape
        tok_count = seq_count * seq_len
        kv_rank = w_kv_down.shape[COL] - ROPE_DIM
        n_dev = mesh.shape['fsdp']
        my_dev = lax.axis_index('fsdp')
        side = lax.rem(my_dev, PAIR)
        n_slots = n_dev * BASE_CAP + HEAVY_CAP
        flat_ids = tok_ids.reshape(tok_count)
        grad_rows = grad_out.reshape(tok_count, d_model)

        owner, owner_rank, is_first, counts = plan_ids(flat_ids, vocab_dev, n_dev)

        def token_slots(turn):
            return slots_of(owner, owner_rank, my_dev, n_dev, turn)

        note = [slot_list(flat_ids, token_slots(0), is_first, n_slots), flat_ids, counts, norm_gain, kv_gain]
        note = jnp.concatenate([piece.astype(jnp.float32) for piece in note])
        note = jnp.pad(note, (0, -note.shape[ROW] % 128))
        notes = lax.all_gather(note, 'fsdp')
        ends = [0]
        for size in (n_slots, tok_count, n_dev, norm_gain.shape[ROW], kv_gain.shape[ROW]):
            ends.append(ends[-1] + size)
        all_slots, all_ids, all_counts, all_gains, all_kv_gains = (notes[:, low:high] for low, high in zip(ends[:-1], ends[1:]))
        all_slots, all_ids, all_counts = (piece.astype(jnp.int32) for piece in (all_slots, all_ids, all_counts))
        gain_f32, kv_gain_f32 = all_gains.reshape(-1), all_kv_gains.reshape(-1)
        caps = owner_cap(jnp.arange(n_dev))
        turns = jnp.max((all_counts + caps - 1) // caps)

        w_out_full = lax.all_gather(w_out, 'fsdp', tiled=True)
        query_shard, down_shard = after(tuple(arrange_weights(w_query, w_kv_down)), notes)
        w_query_full = lax.all_gather(query_shard, 'fsdp', tiled=True)
        w_down_full = lax.all_gather(down_shard, 'fsdp', tiled=True)

        def turn_lists(turn):
            def one_dev(ids, dev, turn):
                its_owner, its_rank, its_first, _ = plan_ids(ids, vocab_dev, n_dev)
                return slot_list(ids, slots_of(its_owner, its_rank, dev, n_dev, turn), its_first, n_slots)

            ids, turn = lax.optimization_barrier((all_ids, jnp.asarray(turn, jnp.int32)))
            return wanted_lists(jax.vmap(one_dev, (0, 0, None))(ids, jnp.arange(n_dev), turn), my_dev, n_dev)

        def spread_of(turn):
            return (token_slots(turn)[:, NEW] == jnp.arange(n_slots)[NEW, :]).astype(jnp.bfloat16)

        def fetch_rows(lists):
            return swap_rows(pick_rows(emb_table, lists, my_dev), n_dev)

        def expand(turn, slot_rows):
            return jnp.dot(spread_of(turn), slot_rows, preferred_element_type=jnp.float32).astype(jnp.bfloat16)

        def expand_more(step, have):
            rows = lax.fori_loop(1, turns, lambda turn, have: have + expand(turn, fetch_rows(turn_lists(turn))), expand(0, slot_rows))
            normed = rms_scale(rows, gain_f32)
            return (rows, normed) + side_blocks(normed, side, n_dev)

        lists = wanted_lists(all_slots, my_dev, n_dev)
        work = (token_slots(0).reshape(1, tok_count), grad_rows, w_out_full)
        slot_rows, slot_dy, d_mix = swap_rows(pick_rows(emb_table, lists, my_dev), n_dev, work)
        many = (turns > 1).astype(jnp.int32)
        first_rows = tuple(expand_rows(token_slots(0), slot_rows, gain_f32, side, n_dev))
        tok_rows, normed, x_own, x_give = lax.fori_loop(0, many, expand_more, first_rows)

        w_up_full = lax.all_gather(after(w_kv_up, slot_rows), 'fsdp', tiled=True)
        down = jnp.dot(normed, w_down_full, preferred_element_type=jnp.float32).astype(jnp.bfloat16)
        latent, latent_pull = jax.vjp(rms_scale, down[:, :kv_rank], kv_gain_f32)
        kv_all = jnp.dot(latent, w_up_full, preferred_element_type=jnp.float32).astype(jnp.bfloat16)
        q_all = jnp.dot(normed, w_query_full, preferred_element_type=jnp.float32).astype(jnp.bfloat16)
        x_both = (x_own, hop_send(x_give, 1, n_dev))
        dy_both = (grad_rows, hop_send(grad_rows, 1, n_dev))
        latent_own, latent_give = side_blocks(latent, side, n_dev)
        latent_both = (latent_own, hop_send(latent_give, 1, n_dev))
        mix, mix_own, mix_give, d_query, d_up, d_pe = attend_pairs(q_all, kv_all, down[:, kv_rank:], d_mix, seq_count, side)

        mix_both = (mix_own, hop_send(mix_give, 1, n_dev))
        dq_both = (d_query, hop_send(d_query, 1, n_dev))
        dup_both = (d_up, hop_send(d_up, 1, n_dev))
        d_latent = lax.dot_general(d_up, w_up_full, COL_DIMS, preferred_element_type=jnp.float32).astype(jnp.bfloat16)
        d_w_out = grad_rows_of((after(mix_both[0], d_latent), mix_both[1]), dy_both)
        g_out = side_scatter(d_w_out, n_dev)
        d_ckv, d_kv_gain = latent_pull(after(d_latent, d_w_out))
        d_down = jnp.concatenate([d_ckv, d_pe], axis=COL)
        d_normed = lax.dot_general(after(d_query, d_w_out), w_query_full, COL_DIMS, preferred_element_type=jnp.float32)
        d_normed = d_normed + lax.dot_general(d_down, w_down_full, COL_DIMS, preferred_element_type=jnp.float32)
        d_normed = d_normed.astype(jnp.bfloat16)
        parts = fold_rows(token_slots(0), d_normed, slot_dy, slot_rows, gain_f32, n_dev)
        pieces = permute_rows(parts, n_dev)

        d_w_up = grad_rows_of((after(latent_both[0], *parts), latent_both[1]), dup_both)
        g_up = side_scatter(d_w_up, n_dev)
        toks_f32 = after(tok_rows, d_w_up).astype(jnp.float32)
        gains = jnp.concatenate([gain_back(toks_f32, d_normed.astype(jnp.float32)), d_kv_gain])
        gains = gains + hop_send(gains, 1, n_dev)
        down_both = (after(d_down, d_w_up), hop_send(d_down, 1, n_dev))
        d_w_down = grad_rows_of(x_both, down_both, LANES)
        gain_col = lax.dynamic_index_in_dim(gains[:d_model].reshape(-1, 2, d_model // n_dev), side, 1, False)
        kv_gain_col = lax.dynamic_index_in_dim(gains[d_model:].reshape(-1, 2, kv_rank // n_dev), side, 1, False)
        kv_gain_col = jnp.pad(kv_gain_col, ((0, 0), (0, (d_model - kv_rank) // n_dev)))
        col_at = jnp.arange(d_w_down.shape[COL])[NEW, :]
        gain_at, kv_gain_at = kv_rank + HALF_ROPE, kv_rank + ROPE_DIM + HALF_ROPE
        d_w_down = jnp.where(col_at == gain_at, gain_col.reshape(-1, 1), jnp.where(col_at == kv_gain_at, kv_gain_col.reshape(-1, 1), d_w_down))
        g_down = side_scatter(d_w_down, n_dev)
        d_w_query = grad_rows_of((after(x_both[0], d_w_down), x_both[1]), dq_both, 2 * PAIR_DIM, heads_pick())
        block_out = (toks_f32 + jnp.dot(after(mix, d_w_query), w_out_full, preferred_element_type=jnp.float32)).astype(jnp.bfloat16)
        first_plan = table_plan(after(lists, d_w_query), my_dev, vocab_dev)
        g_query = side_scatter(after(d_w_query, pieces, block_out), n_dev)

        def many_turns(step, table):
            d_rows = grad_rows.astype(jnp.float32) + norm_back(tok_rows.astype(jnp.float32), d_normed.astype(jnp.float32), gain_f32)

            def add_turn(turn, table):
                slot_grads = lax.dot_general(spread_of(turn).astype(jnp.float32), d_rows, ROW_DIMS, precision=lax.Precision.HIGHEST, preferred_element_type=jnp.float32)
                return write_table(return_rows(slot_grads, n_dev), table_plan(turn_lists(turn), my_dev, vocab_dev), my_dev, vocab_dev, jnp.float32, table)

            return lax.fori_loop(0, turns, add_turn, jnp.zeros((vocab_dev, d_model), jnp.float32)).astype(jnp.bfloat16)

        grad_table = lax.fori_loop(0, many, many_turns, write_table(pieces, first_plan, my_dev, vocab_dev, jnp.bfloat16))
        g_pe = [g_down[:, kv_rank:kv_rank + HALF_ROPE], g_down[:, kv_rank + ROPE_DIM:kv_rank + ROPE_DIM + HALF_ROPE]]
        grads = (g_down[:, gain_at], g_query, jnp.concatenate([g_down[:, :kv_rank]] + g_pe, axis=COL), g_down[:kv_gain.shape[ROW], kv_gain_at], g_up, g_out)
        return (block_out.reshape(seq_count, seq_len, d_model), grad_table) + grads

    return jax.shard_map(device_step, mesh=mesh, in_specs=(tok_spec, seq_spec, mat_spec, vec_spec, mat_spec, mat_spec, vec_spec, mat_spec, mat_spec), out_specs=(seq_spec, tok_spec, part_vec, tok_spec, tok_spec, part_vec, tok_spec, tok_spec), check_vma=False)
```
